256 devices in a mesh: lon: 64 (over x, z, core), ens: 4 (over y).
Axes of the slice: x: 4, y: 4, z: 8, core: 2. Of those that a mesh axis runs over, the one named last changes fastest.
Arguments:
- perturb: bfloat16 [32, 256, 4096], P(None, 'lon'), may hold values from -6 to 6
- eig_table: bfloat16 [24, 256, 4096], P(None, 'lon'), may hold values from -8 to 8
- mode_index: int32 [16], replicated, may hold values from 0 to 23, as said below
- mean_state: bfloat16 [256, 4096], P('lon'), may hold values from -6 to 6
- obs_col: int32 [524288], P('lon'), may hold values from 0 to 3
- obs_row: int32 [524288], P('lon'), may hold values from 0 to 4095
- obs_frac: float32 [524288], P('lon'), may hold values from 0 to 1
- obs_value: float32 [524288], P('lon'), may hold values from -20 to 20
- obs_sigma: float32 [524288], P('lon'), may hold values from 0.5 to 2
Outputs:
- analysis: bfloat16 [512, 256, 4096], P('ens', 'lon')
- increment: float32 [256, 4096], P('lon')
The draws below stay inside these ranges and needn't reach their ends.
Inputs may be any that keep to these rules, and one draw needn't show every extreme that they name: `mode_index`: distinct entries.
All inputs are finite; a program needn't handle non-finite values.
Results may differ from the reference program's by a relative error of at most 0.009.
Values may be sent and summed in bfloat16 or wider, within the bound.
No kernel may reach another device: no remote copies, remote signals or barrier semaphores. Data moves between devices by JAX's collectives and lax.ppermute only.
A program may use at most 128 MiB of HBM per device.

```python
import math
import jax
import jax.numpy as jnp
from jax import lax

MEMBERS = 32
MODES = 16
TABLE = 24
NLAT = 4096
LON_DEV = 4
OBS_DEV = 8192
COLUMNS = 512
NLON = 256
NOBS = 524288
N_LON = 64


def draw_mode_index(key, part):
    return jax.random.permutation(key, TABLE)[:MODES].astype(jnp.int32)


def draw_eig_table(key, part):
    subkeys = jax.random.split(key, 3)
    own_part = jax.random.normal(subkeys[0], (TABLE, NLON, NLAT), jnp.float32)
    common = 0.7 * jax.random.normal(subkeys[2], (1, NLON, NLAT), jnp.float32)
    result = own_part + common
    return jnp.clip(result, -8.0, 8.0).astype(jnp.bfloat16)


def draw_obs_value(key, part):
    subkeys = jax.random.split(key, 3)
    noise_draw = jax.random.normal(subkeys[0], (NOBS,), jnp.float32)
    result = noise_draw
    return jnp.clip(result, -20.0, 20.0)


def set_ends(drawn, rng, low, largest):
    index_at = [jax.random.randint(jax.random.fold_in(rng, axis), (), 0, length) for axis, length in enumerate(drawn.shape)]
    longest = drawn.shape.index(max(drawn.shape))
    neighbour = index_at[:longest] + [(index_at[longest] + 1) % drawn.shape[longest]] + index_at[longest + 1:]
    return drawn.at[tuple(index_at)].set(low).at[tuple(neighbour)].set(largest)


def block_levels(key, dims, pieces, low, top_value):
    loudness, own = 1.0, jax.random.fold_in(key, 6)
    for dim, shards_of in pieces:
        heights = jnp.exp(jax.random.uniform(jax.random.fold_in(own, dim), (shards_of,), jnp.float32, low / len(pieces), top_value / len(pieces)))
        loudness = loudness * jnp.repeat(heights, dims[dim] // shards_of).reshape([-1 if axis == dim else 1 for axis in range(len(dims))])
    return loudness


def noise(key, extent, width, bound, cuts=(), kind=jnp.bfloat16):
    values = jax.random.normal(key, extent, jnp.float32) * width
    if len(cuts) > 0:
        values = block_levels(key, extent, cuts, -0.22, 0.18) * values
    return jnp.clip(values, min=-bound, max=bound).astype(kind)


def setup_inputs(seed: int = 0) -> dict:
    key_list = jax.random.split(jax.random.key(seed), 10)
    return {
        "perturb": noise(key_list[0], (MEMBERS, NLON, NLAT), 1.0, 6.0, ((1, 64),)),
        "eig_table": draw_eig_table(jax.random.fold_in(key_list[9], 71), 0),
        "mode_index": draw_mode_index(jax.random.fold_in(key_list[9], 71), 0),
        "mean_state": noise(key_list[3], (NLON, NLAT), 1.0, 6.0, ((0, 64),)),
        "obs_col": set_ends(jax.random.randint(key_list[4], (NOBS,), 0, LON_DEV), jax.random.fold_in(key_list[4], 1), 0, LON_DEV - 1).astype(jnp.int32),
        "obs_row": set_ends(jax.random.randint(key_list[5], (NOBS,), 0, NLAT), jax.random.fold_in(key_list[5], 1), 0, NLAT - 1).astype(jnp.int32),
        "obs_frac": jnp.clip(1.0 * jax.random.uniform(key_list[6], (NOBS,), jnp.float32) ** block_levels(key_list[6], (NOBS,), ((0, 64),), -0.2, 0.2), 0.0, 1.0),
        "obs_value": draw_obs_value(jax.random.fold_in(key_list[9], 71), 0),
        "obs_sigma": jnp.clip(jnp.exp(math.log(2.0) - 1.3862944 * jax.random.uniform(key_list[8], (NOBS,), jnp.float32) ** block_levels(key_list[8], (NOBS,), ((0, 64),), -0.2, 0.2)), 0.5, 2.0),
    }


def reference(perturb, eig_table, mode_index, mean_state, obs_col, obs_row, obs_frac, obs_value, obs_sigma):
    inv_root = 1.0 / jnp.sqrt(jnp.float32(MEMBERS - 1))
    obs_scale = jnp.sqrt(jnp.float32(4 * MEMBERS) / jnp.float32(NOBS))
    chosen = eig_table[mode_index].astype(jnp.float32)
    member_rows = perturb.astype(jnp.float32)
    mean_rows = mean_state.astype(jnp.float32)

    def band_terms(band_index):
        first_obs = band_index * OBS_DEV
        band_cols = lax.dynamic_slice_in_dim(obs_col, first_obs, OBS_DEV)
        band_rows = lax.dynamic_slice_in_dim(obs_row, first_obs, OBS_DEV)
        fraction = lax.dynamic_slice_in_dim(obs_frac, first_obs, OBS_DEV)
        observed = lax.dynamic_slice_in_dim(obs_value, first_obs, OBS_DEV)
        obs_error = lax.dynamic_slice_in_dim(obs_sigma, first_obs, OBS_DEV)
        lon_here = (band_index * LON_DEV + band_cols).astype(jnp.int32)
        lon_next = ((lon_here + 1) % NLON).astype(jnp.int32)
        pert_here = member_rows[:, lon_here, band_rows]
        pert_next = member_rows[:, lon_next, band_rows]
        mode_here = chosen[:, lon_here, band_rows]
        mode_next = chosen[:, lon_next, band_rows]
        blended = (1.0 - fraction) * mode_here[:, None, :] * pert_here[None] + fraction * mode_next[:, None, :] * pert_next[None]
        obs_columns = (blended * (obs_scale * inv_root / obs_error)).reshape(COLUMNS, OBS_DEV)
        normed = (observed - ((1.0 - fraction) * mean_rows[lon_here, band_rows] + fraction * mean_rows[lon_next, band_rows])) / obs_error
        rounded = obs_columns.astype(jnp.bfloat16)
        gram_part = jnp.dot(rounded.astype(jnp.float32), rounded.T.astype(jnp.float32), preferred_element_type=jnp.float32)
        gain_part = jnp.dot(obs_columns, normed, precision=lax.Precision.HIGHEST)
        return (gram_part, gain_part, jnp.sum(normed * normed))
    gram_parts, gain_parts, square_parts = lax.map(band_terms, jnp.arange(N_LON, dtype=jnp.int32))
    gram_matrix = lax.optimization_barrier(jnp.sum(gram_parts, axis=0))
    gain_vector = lax.optimization_barrier(jnp.sum(gain_parts, axis=0))
    square_sum = jnp.sum(square_parts)
    prior_scale = 2.0 / (1.0 + square_sum / NOBS)
    identity = jnp.eye(COLUMNS, dtype=jnp.float32)
    factor_lower = jnp.linalg.cholesky(identity + prior_scale * gram_matrix)
    inverse = lax.linalg.triangular_solve(factor_lower, identity, left_side=True, lower=True)
    inner = jnp.dot(inverse, gain_vector, precision=lax.Precision.HIGHEST)
    weights = jnp.sqrt(prior_scale) * jnp.dot(inverse.T, inner, precision=lax.Precision.HIGHEST)
    inverse_rounded = inverse.astype(jnp.bfloat16)
    weights_rounded = weights.astype(jnp.bfloat16)

    def band_transform(band_index):
        first_lon = band_index * LON_DEV
        band_members = lax.dynamic_slice_in_dim(member_rows, first_lon, LON_DEV, 1)
        band_modes = lax.dynamic_slice_in_dim(chosen, first_lon, LON_DEV, 1)
        columns = (band_modes[:, None] * band_members[None] * inv_root).reshape(COLUMNS, LON_DEV * NLAT).astype(jnp.bfloat16)
        increment_band = jnp.sqrt(prior_scale) * jnp.dot(weights_rounded.astype(jnp.float32), columns.astype(jnp.float32), preferred_element_type=jnp.float32)
        product = jnp.dot(inverse_rounded.astype(jnp.float32), columns.astype(jnp.float32), preferred_element_type=jnp.float32)
        analysis_band = (jnp.sqrt(prior_scale * (MEMBERS - 1)) * product).astype(jnp.bfloat16)
        return (analysis_band.reshape(COLUMNS, LON_DEV, NLAT), increment_band.reshape(LON_DEV, NLAT))
    analysis_bands, increment_bands = lax.map(band_transform, jnp.arange(N_LON, dtype=jnp.int32))
    analysis = jnp.transpose(analysis_bands, (1, 0, 2, 3)).reshape(COLUMNS, NLON, NLAT)
    increment = increment_bands.reshape(NLON, NLAT)
    return (analysis, increment)
```

```python
import jax
import jax.numpy as jnp
from jax import lax
from jax.experimental import pallas as pl
from jax.experimental.pallas import tpu as pltpu
from jax.sharding import PartitionSpec as P


F32 = jnp.float32
BF16 = jnp.bfloat16
HIGHEST = lax.Precision.HIGHEST
SMEM = pltpu.SMEM
VMEM = pltpu.VMEM

BLOCK = 128
SLOT = 64
NT = (((1,), (1,)), ((), ()))
TN = (((0,), (0,)), ((), ()))


def vmem(*shape_dtype):
    return pl.BlockSpec(memory_space=VMEM)


def smem():
    return pl.BlockSpec(memory_space=SMEM)


def table_body(picker_ref, pert_ref, eig_ref, mean_ref, table_ref):
    members, lon_cols, lat = pert_ref.shape
    modes = picker_ref.shape[0]
    picker = picker_ref[...]
    for j in range(lon_cols):
        base = j * SLOT
        table_ref[base : base + members, :] = pert_ref[:, j, :]
        picked = jnp.dot(picker, eig_ref[:, j, :], preferred_element_type=F32)
        table_ref[base + members : base + members + modes, :] = picked.astype(BF16)
        rest = SLOT - members - modes
        mean_row = mean_ref[j : j + 1, :].astype(F32)
        first = lax.broadcasted_iota(jnp.int32, (rest, lat), 0) == 0
        table_ref[base + members + modes : base + SLOT, :] = jnp.where(
            first, jnp.broadcast_to(mean_row, (rest, lat)), 0.0
        ).astype(BF16)


def one_hot_dot(table_ref, rows, width):
    lat = table_ref.shape[1]
    chunk = 512
    total = None
    for start in range(0, lat, chunk):
        place = lax.broadcasted_iota(jnp.int32, (chunk, width), 0) + start
        hot = jnp.where(place == rows, 1.0, 0.0).astype(BF16)
        part = jnp.dot(table_ref[:, start : start + chunk], hot, preferred_element_type=F32)
        total = part if total is None else total + part
    return total


def gather_body(obs_ref, table_ref, out_ref):
    rows = obs_ref[1:2, :].astype(jnp.int32)
    out_ref[...] = one_hot_dot(table_ref, rows, out_ref.shape[1]).astype(BF16)


def gram_body(sizes, place_ref, obs_ref, here_ref, edge_ref, keep_ref, send_ref, columns, packed):
    members, modes, obs_scale_root, lon_cols, pieces_y, pieces_x = sizes
    step = pl.program_id(0)
    steps = pl.num_programs(0)
    width = obs_ref.shape[1]
    count = members * modes
    col = obs_ref[0:1, :]
    rows = obs_ref[1:2, :].astype(jnp.int32)
    fraction = obs_ref[2:3, :]
    observed = obs_ref[3:4, :]
    obs_error = obs_ref[4:5, :]
    edge = one_hot_dot(edge_ref, rows, width)
    here = jnp.zeros((SLOT, width), F32)
    beyond = jnp.zeros((SLOT, width), F32)
    for j in range(lon_cols):
        pick = col == j
        here = jnp.where(pick, here_ref[j * SLOT : (j + 1) * SLOT, :].astype(F32), here)
        if j + 1 < lon_cols:
            nxt = here_ref[(j + 1) * SLOT : (j + 2) * SLOT, :].astype(F32)
        else:
            nxt = edge
        beyond = jnp.where(pick, nxt, beyond)
    weight = obs_scale_root / obs_error
    first_weight = (1.0 - fraction) * weight
    second_weight = fraction * weight
    pert_here = here[:members]
    pert_next = beyond[:members]
    mode_here = here[members : members + modes] * first_weight
    mode_next = beyond[members : members + modes] * second_weight
    mean_at = members + modes
    normed = (
        observed
        - ((1.0 - fraction) * here[mean_at : mean_at + 1] + fraction * beyond[mean_at : mean_at + 1])
    ) / obs_error
    at = pl.multiple_of(step * width, 128)
    for mode in range(modes):
        block = mode_here[mode : mode + 1] * pert_here + mode_next[mode : mode + 1] * pert_next
        columns[mode * members : (mode + 1) * members, pl.ds(at, width)] = block.astype(BF16)
    normed_high = normed.astype(BF16).astype(F32)
    normed_low = normed - normed_high
    which = lax.broadcasted_iota(jnp.int32, (16, width), 0)
    extra = jnp.where(
        which == 0,
        jnp.broadcast_to(normed_high, (16, width)),
        jnp.where(which == 1, jnp.broadcast_to(normed_low, (16, width)), 0.0),
    )
    columns[count : count + 16, pl.ds(at, width)] = extra.astype(BF16)

    @pl.when(step == steps - 1)
    def _():
        everything = columns[...]
        blocks = count // BLOCK
        tail = lax.dot_general(
            everything[count:], everything, NT, preferred_element_type=F32
        )
        gain = tail[0:1, :count] + tail[1:2, :count]
        own = everything[count:].astype(F32)
        total_normed = own[0:1] + own[1:2]
        square_sum = jnp.sum(total_normed * total_normed)
        row_at = lax.broadcasted_iota(jnp.int32, (BLOCK, BLOCK), 0)
        lane_at = lax.broadcasted_iota(jnp.int32, (BLOCK, BLOCK), 1)
        at_block = 0
        for i in range(blocks):
            strip = lax.dot_general(
                everything[i * BLOCK : (i + 1) * BLOCK],
                everything[: (i + 1) * BLOCK],
                NT,
                preferred_element_type=F32,
            )
            for j in range(i + 1):
                block = strip[:, j * BLOCK : (j + 1) * BLOCK]
                if i == j:
                    part = gain[:, i * BLOCK : (i + 1) * BLOCK]
                    turned = pltpu.roll(jnp.broadcast_to(part, (8, BLOCK)), SLOT, axis=1)
                    upper = lane_at >= SLOT
                    block = jnp.where((row_at == 0) & upper, jnp.broadcast_to(turned[0:1], (BLOCK, BLOCK)), block)
                    block = jnp.where(
                        (row_at == 1) & upper, jnp.broadcast_to(part, (BLOCK, BLOCK)), block
                    )
                    if i == 0:
                        block = jnp.where((row_at == 2) & upper, square_sum, block)
                packed[at_block * BLOCK : (at_block + 1) * BLOCK, :] = block
                at_block += 1
        core, own_y, own_x = place_ref[0], place_ref[1], place_ref[2]
        pieces = 2 * pieces_y * pieces_x
        size = packed.shape[0] // pieces
        half = pieces // 2
        for side, out_ref in ((0, keep_ref), (1, send_ref)):
            for slot in range(half):
                y = lax.rem(own_y + slot // pieces_x, pieces_y)
                x = lax.rem(own_x + slot % pieces_x, pieces_x)
                c = core if side == 0 else 1 - core
                piece = (c * pieces_y + y) * pieces_x + x
                out_ref[slot * size : (slot + 1) * size, :] = packed[
                    pl.ds(pl.multiple_of(piece * size, 8), size), :
                ]


def invert_diagonal(work, base):
    tiles = BLOCK // 8
    lane = lax.broadcasted_iota(jnp.int32, (8, BLOCK), 1)
    sub = lax.broadcasted_iota(jnp.int32, (8, BLOCK), 0)
    rows = [work[pl.ds(base + 8 * t, 8), :] for t in range(tiles)]
    for t in range(tiles):
        at = 8 * t
        mine = rows[t]
        spread = [
            [
                None if j > i else jnp.broadcast_to(mine[i : i + 1, at + j : at + j + 1], (8, BLOCK))
                for j in range(8)
            ]
            for i in range(8)
        ]
        outside = {
            s: [jnp.broadcast_to(rows[s][:, at + j : at + j + 1], (8, BLOCK)) for j in range(8)]
            for s in range(t + 1, tiles)
        }
        pivots = []
        unit = [[None] * 8 for _ in range(8)]
        current = [list(row) for row in spread]
        for k in range(8):
            recip = 1.0 / current[k][k]
            pivots.append(recip)
            for i in range(k + 1, 8):
                unit[i][k] = current[i][k] * recip
            for i in range(k + 1, 8):
                for j in range(k + 1, i + 1):
                    current[i][j] = current[i][j] - unit[i][k] * current[j][k]
        inv = [[None] * 8 for _ in range(8)]
        for j in range(8):
            for i in range(j + 1, 8):
                value = -unit[i][j]
                for k in range(j + 1, i):
                    value = value - unit[i][k] * inv[k][j]
                inv[i][j] = value
        clear = (lane >= at) & (lane < at + 8)
        base_row = jnp.where(clear, jnp.where(lane - at == sub, 1.0, 0.0), mine)
        spread_rows = [jnp.broadcast_to(base_row[k : k + 1, :], (8, BLOCK)) for k in range(8)]
        done = [spread_rows[0]]
        for i in range(1, 8):
            value = spread_rows[i]
            for k in range(i):
                value = value + inv[i][k] * spread_rows[k]
            done.append(value)
        scaled = [done[i] * pivots[i] for i in range(8)]
        solved = []
        for j in range(8):
            value = scaled[j]
            for i in range(j + 1, 8):
                value = value + inv[i][j] * scaled[i]
            solved.append(value)
        for s in range(t + 1, tiles):
            left = jnp.where(clear, 0.0, rows[s])
            for j in range(8):
                left = left - outside[s][j] * solved[j]
            rows[s] = left
        out = done[0] * lax.rsqrt(current[0][0])
        for i in range(1, 8):
            out = jnp.where(sub == i, done[i] * lax.rsqrt(current[i][i]), out)
        rows[t] = jnp.where(lane < at + 8, out, 0.0)
    return rows


def factor_body(sizes, place_ref, parts_ref, inverse_ref, scale_ref, packed, work, full):
    pieces_y, pieces_x, obs_total, members = sizes
    core, own_y, own_x = place_ref[0], place_ref[1], place_ref[2]
    pieces = 2 * pieces_y * pieces_x
    size = packed.shape[0] // pieces
    half = pieces // 2
    for side in range(2):
        for slot in range(half):
            y = lax.rem(own_y + slot // pieces_x, pieces_y)
            x = lax.rem(own_x + slot % pieces_x, pieces_x)
            c = core if side == 0 else 1 - core
            piece = (c * pieces_y + y) * pieces_x + x
            packed[pl.ds(pl.multiple_of(piece * size, 8), size), :] = parts_ref[
                (side * half + slot) * size : (side * half + slot + 1) * size, :
            ].astype(F32)
    count = full.shape[0]
    blocks = count // BLOCK
    row_at = lax.broadcasted_iota(jnp.int32, (BLOCK, BLOCK), 0)
    lane_at = lax.broadcasted_iota(jnp.int32, (BLOCK, BLOCK), 1)
    square_sum = packed[2:3, SLOT : SLOT + 1]
    prior_scale = 2.0 / (1.0 + square_sum / obs_total)
    gains = []
    at_block = 0
    for i in range(blocks):
        for j in range(i + 1):
            block = packed[at_block * BLOCK : (at_block + 1) * BLOCK, :]
            at_block += 1
            if i == j:
                first = pltpu.roll(jnp.broadcast_to(block[0:1], (8, BLOCK)), SLOT, axis=1)[0:1]
                gains.append(jnp.where(lane_at[0:1] < SLOT, first, block[1:2]))
                block = jnp.where(row_at >= lane_at, block, block.T)
                block = block * prior_scale + jnp.where(row_at == lane_at, 1.0, 0.0)
                full[i * BLOCK : (i + 1) * BLOCK, j * BLOCK : (j + 1) * BLOCK] = block
            else:
                block = block * prior_scale
                full[i * BLOCK : (i + 1) * BLOCK, j * BLOCK : (j + 1) * BLOCK] = block
                full[j * BLOCK : (j + 1) * BLOCK, i * BLOCK : (i + 1) * BLOCK] = block.T
    for b in range(blocks):
        low, high = b * BLOCK, (b + 1) * BLOCK
        rows = invert_diagonal(full.at[:, low:high], low)
        diag = jnp.concatenate(rows, axis=0)
        if b > 0:
            left = jnp.dot(diag, full[low:high, :low], precision=HIGHEST, preferred_element_type=F32)
        if high < count:
            right = jnp.dot(diag, full[low:high, high:], precision=HIGHEST, preferred_element_type=F32)
            for i in range(b + 1, blocks):
                ilow, ihigh = i * BLOCK, (i + 1) * BLOCK
                factor = right[:, ilow - high : ihigh - high]
                full[ilow:ihigh, high:] = full[ilow:ihigh, high:] - lax.dot_general(
                    factor, right, TN, precision=HIGHEST, preferred_element_type=F32
                )
                if b > 0:
                    full[ilow:ihigh, :low] = full[ilow:ihigh, :low] - lax.dot_general(
                        factor, left, TN, precision=HIGHEST, preferred_element_type=F32
                    )
                full[ilow:ihigh, low:high] = -lax.dot_general(
                    factor, diag, TN, precision=HIGHEST, preferred_element_type=F32
                )
            full[low:high, high:] = jnp.zeros((BLOCK, count - high), F32)
        full[low:high, low:high] = diag
        if b > 0:
            full[low:high, :low] = left
    inverse = full[...]
    gain = jnp.broadcast_to(jnp.concatenate(gains, axis=1), (8, count))
    inner = lax.dot_general(gain, inverse, NT, precision=HIGHEST, preferred_element_type=F32)
    weights = jnp.dot(inner, inverse, precision=HIGHEST, preferred_element_type=F32)
    weights = weights * jnp.sqrt(prior_scale)
    own_rows = inverse_ref.shape[0] - 16
    inverse_ref[:own_rows, :] = full[pl.ds(pl.multiple_of(own_y * own_rows, 8), own_rows), :].astype(BF16)
    inverse_ref[own_rows:, :] = jnp.broadcast_to(weights[0:1], (16, count)).astype(BF16)
    scale_ref[...] = jnp.broadcast_to(prior_scale, scale_ref.shape)


def apply_body(inv_root, picker_ref, scale_ref, inverse_ref, pert_ref, eig_ref, analysis_ref, increment_ref, columns):
    members, lon_cols, width = pert_ref.shape
    modes = picker_ref.shape[0]
    own_rows = analysis_ref.shape[0]
    prior_scale = scale_ref[0:1, 0:1]
    analysis_scale = jnp.sqrt(prior_scale * (members - 1)) * inv_root
    increment_scale = jnp.sqrt(prior_scale) * inv_root
    results = []
    for j in range(lon_cols):
        own = pert_ref[:, j, :]
        picked = jnp.dot(picker_ref[...], eig_ref[:, j, :], preferred_element_type=F32).astype(BF16)
        for mode in range(modes):
            columns[mode * members : (mode + 1) * members, :] = picked[mode : mode + 1] * own
        product = jnp.dot(inverse_ref[...], columns[...], preferred_element_type=F32)
        analysis_ref[:, j, :] = (product[:own_rows] * analysis_scale).astype(BF16)
        increment_ref[j : j + 1, :] = product[own_rows : own_rows + 1] * increment_scale


def local(perturb, eig_table, mode_index, mean_state, obs_col, obs_row, obs_frac, obs_value, obs_sigma):
    members, lon_cols, lat = perturb.shape
    table_rows = eig_table.shape[0]
    modes = mode_index.shape[0]
    obs_local = obs_col.shape[0]
    lon_devices = lax.axis_size("lon")
    ens_devices = lax.axis_size("ens")
    obs_total = obs_local * lon_devices
    count = modes * members
    obs_own = obs_local // ens_devices
    own_y = lax.axis_index("ens")
    lon = lax.axis_index("lon")
    xs = 4
    zs = lon_devices // (2 * xs)
    core = lon % 2
    own_x = lon // (2 * zs)
    place = jnp.stack([core, own_y, own_x]).astype(jnp.int32)
    inv_root = 1.0 / float(members - 1) ** 0.5
    obs_scale = (4.0 * members / obs_total) ** 0.5

    picker = (mode_index[:, None] == jnp.arange(table_rows, dtype=jnp.int32)[None, :]).astype(BF16)
    table = pl.pallas_call(
        table_body,
        out_shape=jax.ShapeDtypeStruct((lon_cols * SLOT, lat), BF16),
        in_specs=[vmem()] * 4,
        out_specs=vmem(),
        name="table",
    )(picker, perturb, eig_table, mean_state)
    back = [(source, (source - 1) % lon_devices) for source in range(lon_devices)]
    edge_rows = 56
    edge = lax.ppermute(table[:edge_rows], "lon", back)
    edge = jnp.pad(edge, ((0, SLOT - edge_rows), (0, 0)))

    def own_part(value):
        return lax.dynamic_slice_in_dim(value, own_y * obs_own, obs_own).astype(F32)

    zero = jnp.zeros((obs_own,), F32)
    obs = jnp.stack(
        [own_part(v) for v in (obs_col, obs_row, obs_frac, obs_value, obs_sigma)] + [zero] * 3
    )
    width = 256
    steps = obs_own // width
    here = pl.pallas_call(
        gather_body,
        grid=(steps,),
        out_shape=jax.ShapeDtypeStruct((lon_cols * SLOT, obs_own), BF16),
        in_specs=[pl.BlockSpec((8, width), lambda g: (0, g)), vmem()],
        out_specs=pl.BlockSpec((lon_cols * SLOT, width), lambda g: (0, g)),
        cost_estimate=pl.CostEstimate(flops=2 * lat * obs_own * lon_cols * SLOT, bytes_accessed=4 << 20, transcendentals=0),
        name="gather",
    )(obs, table)
    blocks = count // BLOCK
    packed_rows = blocks * (blocks + 1) // 2 * BLOCK
    half = packed_rows // 2
    ys = ens_devices
    keep, send = pl.pallas_call(
        lambda *refs: gram_body((members, modes, obs_scale * inv_root, lon_cols, ys, xs), *refs),
        grid=(steps,),
        out_shape=[jax.ShapeDtypeStruct((half, BLOCK), F32)] * 2,
        in_specs=[
            smem(),
            pl.BlockSpec((8, width), lambda g: (0, g)),
            pl.BlockSpec((lon_cols * SLOT, width), lambda g: (0, g)),
            vmem(),
        ],
        out_specs=[vmem(), vmem()],
        scratch_shapes=[VMEM((count + 16, obs_own), BF16), VMEM((packed_rows, BLOCK), F32)],
        name="gram",
    )(place, obs, here, edge)

    def at(x, z, c):
        return ((x % xs) * zs + z % zs) * 2 + c

    spots = [(x, z, c) for x in range(xs) for z in range(zs) for c in range(2)]
    over_core = [(at(x, z, c), at(x, z, 1 - c)) for x, z, c in spots]

    def over_x(d):
        return [(at(x, z, c), at(x + d, z, c)) for x, z, c in spots]

    def over_z(d):
        return [(at(x, z, c), at(x, z + d, c)) for x, z, c in spots]

    def over_y(d):
        return [(y, (y + d) % ys) for y in range(ys)]

    quarter = half // ys
    piece = quarter // xs
    got = lax.ppermute(send, "lon", over_core)
    mine = keep + got
    got = [lax.ppermute(mine[d * quarter : (d + 1) * quarter], "ens", over_y(d)) for d in range(1, ys)]
    mine = mine[:quarter] + sum(got)
    got = [lax.ppermute(mine[d * piece : (d + 1) * piece], "lon", over_x(d)) for d in range(1, xs)]
    mine = mine[:piece] + sum(got)
    got = [lax.ppermute(mine, "lon", over_z(d)) for d in range(1, zs)]
    mine = mine + sum(got)
    got = [lax.ppermute(mine, "lon", over_x(-d)) for d in range(1, xs)]
    mine = jnp.concatenate([mine] + got)
    got = [lax.ppermute(mine, "ens", over_y(-d)) for d in range(1, ys)]
    mine = jnp.concatenate([mine] + got)
    got = lax.ppermute(mine, "lon", over_core)
    parts = jnp.concatenate([mine, got])

    own_columns = count // ens_devices
    inverse, scale = pl.pallas_call(
        lambda *refs: factor_body((ys, xs, float(obs_total), members), *refs),
        out_shape=[
            jax.ShapeDtypeStruct((own_columns + 16, count), BF16),
            jax.ShapeDtypeStruct((8, 128), F32),
        ],
        in_specs=[smem(), vmem()],
        out_specs=[vmem(), vmem()],
        scratch_shapes=[VMEM((packed_rows, BLOCK), F32), VMEM((8, 128), F32), VMEM((count, count), F32)],
        name="factor",
    )(place, parts)
    cells = 512
    analysis, increment = pl.pallas_call(
        lambda *refs: apply_body(inv_root, *refs),
        grid=(lat // cells,),
        out_shape=[
            jax.ShapeDtypeStruct((own_columns, lon_cols, lat), BF16),
            jax.ShapeDtypeStruct((lon_cols, lat), F32),
        ],
        in_specs=[
            vmem(),
            vmem(),
            vmem(),
            pl.BlockSpec((members, lon_cols, cells), lambda g: (0, 0, g)),
            pl.BlockSpec((table_rows, lon_cols, cells), lambda g: (0, 0, g)),
        ],
        out_specs=[
            pl.BlockSpec((own_columns, lon_cols, cells), lambda g: (0, 0, g)),
            pl.BlockSpec((lon_cols, cells), lambda g: (0, g)),
        ],
        scratch_shapes=[VMEM((count, cells), BF16)],
        name="apply",
    )(picker, scale, inverse, perturb, eig_table)
    return (analysis, increment)


def solution(mesh):
    return jax.shard_map(
        local,
        mesh=mesh,
        in_specs=(
            P(None, "lon", None),
            P(None, "lon", None),
            P(),
            P("lon", None),
            P("lon"),
            P("lon"),
            P("lon"),
            P("lon"),
            P("lon"),
        ),
        out_specs=(P("ens", "lon", None), P("lon", None)),
        check_vma=False,
    )
```

```python
import jax
import jax.numpy as jnp
from jax import lax
from jax.experimental import pallas as pl
from jax.experimental.pallas import tpu as pltpu
from jax.sharding import PartitionSpec as P


F32 = jnp.float32
BF16 = jnp.bfloat16
HIGHEST = lax.Precision.HIGHEST
SMEM = pltpu.SMEM
VMEM = pltpu.VMEM

BLOCK = 128
SLOT = 64
NT = (((1,), (1,)), ((), ()))
TN = (((0,), (0,)), ((), ()))


def vmem(*shape_dtype):
    return pl.BlockSpec(memory_space=VMEM)


def smem():
    return pl.BlockSpec(memory_space=SMEM)


def edge_body(index_ref, pert_ref, eig_ref, mean_ref, edge_ref, chosen):
    members = pert_ref.shape[0]
    modes = index_ref.shape[0]
    for mode in range(modes):
        chosen[mode] = eig_ref[index_ref[mode]]
    edge_ref[:members, :] = pert_ref[:, 0, :]
    edge_ref[members : members + modes, :] = chosen[:, 0, :]
    rest = edge_ref.shape[0] - members - modes
    mean_row = mean_ref[0:1, :].astype(F32)
    edge_ref[members + modes :, :] = jnp.broadcast_to(mean_row, (rest, mean_row.shape[1])).astype(BF16)


def table_body(index_ref, pert_ref, eig_ref, table_ref, chosen):
    members, lon_cols, _ = pert_ref.shape
    modes = index_ref.shape[0]
    for mode in range(modes):
        chosen[mode] = eig_ref[index_ref[mode]]
    for j in range(lon_cols):
        base = j * (members + modes)
        table_ref[base : base + members, :] = pert_ref[:, j, :]
        table_ref[base + members : base + members + modes, :] = chosen[:, j, :]


def observe_body(
    sizes, place_ref, col_ref, row_ref, frac_ref, value_ref, sigma_ref, table_ref, edge_ref, mean_ref,
    keep_ref, send_ref, cells, columns, packed,
):
    members, modes, obs_scale_root, width, pieces_y, pieces_x = sizes
    step = pl.program_id(0)
    steps = pl.num_programs(0)
    lon_cols, lat = mean_ref.shape
    slot = members + modes
    count = members * modes
    mean_at = (lon_cols + 1) * slot

    @pl.when(step == 0)
    def _():
        cells[: lon_cols * slot, :] = table_ref[...]
        cells[lon_cols * slot : mean_at, :] = edge_ref[:slot, :]
        rest = cells.shape[0] - mean_at
        line = lax.broadcasted_iota(jnp.int32, (rest, lat), 0)
        means = jnp.zeros((rest, lat), F32)
        for j in range(lon_cols):
            means = jnp.where(line == j, mean_ref[j : j + 1, :].astype(F32), means)
        means = jnp.where(line == lon_cols, edge_ref[slot : slot + 1, :].astype(F32), means)
        cells[mean_at:, :] = means.astype(BF16)

    at = pl.multiple_of((place_ref[1] * steps + step) * width, 128)
    col = col_ref[:, pl.ds(at, width)]
    row = row_ref[:, pl.ds(at, width)]
    fraction = frac_ref[:, pl.ds(at, width)]
    observed = value_ref[:, pl.ds(at, width)]
    obs_error = sigma_ref[:, pl.ds(at, width)]
    high = row // 256
    low = row - high * 256
    spread_high = jnp.broadcast_to(high, (16, width))
    spread_low = jnp.broadcast_to(low, (16, width))
    place = lax.broadcasted_iota(jnp.int32, (256, width), 0).astype(F32).astype(BF16)
    one = jnp.ones((256, width), BF16)
    none = jnp.zeros((256, width), BF16)
    chunk = 4
    found = None
    for start in range(0, lat // 256, chunk):
        parts = []
        for part in range(start, start + chunk):
            wanted = jnp.where(spread_high == part, spread_low, -1).astype(F32).astype(BF16)
            parts.append(jnp.where(place == jnp.concatenate([wanted] * 16, axis=0), one, none))
        hot = jnp.concatenate(parts, axis=0)
        piece = jnp.dot(
            cells[:, start * 256 : (start + chunk) * 256], hot, preferred_element_type=F32
        )
        found = piece if found is None else found + piece
    here = found[:slot]
    beyond = found[slot : 2 * slot]
    mean_here = found[mean_at : mean_at + 1]
    mean_next = found[mean_at + 1 : mean_at + 2]
    for j in range(1, lon_cols):
        pick = col == j
        here = jnp.where(pick, found[j * slot : (j + 1) * slot], here)
        beyond = jnp.where(pick, found[(j + 1) * slot : (j + 2) * slot], beyond)
        mean_here = jnp.where(pick, found[mean_at + j : mean_at + j + 1], mean_here)
        mean_next = jnp.where(pick, found[mean_at + j + 1 : mean_at + j + 2], mean_next)
    weight = obs_scale_root / obs_error
    pert_here = here[:members]
    pert_next = beyond[:members]
    mode_here = here[members:] * ((1.0 - fraction) * weight)
    mode_next = beyond[members:] * (fraction * weight)
    normed = (observed - ((1.0 - fraction) * mean_here + fraction * mean_next)) / obs_error
    own = pl.multiple_of(step * width, 128)
    for mode in range(modes):
        block = mode_here[mode : mode + 1] * pert_here + mode_next[mode : mode + 1] * pert_next
        columns[mode * members : (mode + 1) * members, pl.ds(own, width)] = block.astype(BF16)
    normed_high = normed.astype(BF16).astype(F32)
    normed_low = normed - normed_high
    which = lax.broadcasted_iota(jnp.int32, (16, width), 0)
    extra = jnp.where(
        which == 0,
        jnp.broadcast_to(normed_high, (16, width)),
        jnp.where(which == 1, jnp.broadcast_to(normed_low, (16, width)), 0.0),
    )
    columns[count : count + 16, pl.ds(own, width)] = extra.astype(BF16)

    @pl.when(step == steps - 1)
    def _():
        everything = columns[...]
        blocks = count // BLOCK
        tail = lax.dot_general(
            everything[count:], everything, NT, preferred_element_type=F32
        )
        gain = tail[0:1, :count] + tail[1:2, :count]
        own = everything[count:].astype(F32)
        total_normed = own[0:1] + own[1:2]
        square_sum = jnp.sum(total_normed * total_normed)
        row_at = lax.broadcasted_iota(jnp.int32, (BLOCK, BLOCK), 0)
        lane_at = lax.broadcasted_iota(jnp.int32, (BLOCK, BLOCK), 1)
        at_block = 0
        for i in range(blocks):
            strip = lax.dot_general(
                everything[i * BLOCK : (i + 1) * BLOCK],
                everything[: (i + 1) * BLOCK],
                NT,
                preferred_element_type=F32,
            )
            for j in range(i + 1):
                block = strip[:, j * BLOCK : (j + 1) * BLOCK]
                if i == j:
                    part = gain[:, i * BLOCK : (i + 1) * BLOCK]
                    turned = pltpu.roll(jnp.broadcast_to(part, (8, BLOCK)), SLOT, axis=1)
                    upper = lane_at >= SLOT
                    block = jnp.where((row_at == 0) & upper, jnp.broadcast_to(turned[0:1], (BLOCK, BLOCK)), block)
                    block = jnp.where(
                        (row_at == 1) & upper, jnp.broadcast_to(part, (BLOCK, BLOCK)), block
                    )
                    if i == 0:
                        block = jnp.where((row_at == 2) & upper, square_sum, block)
                packed[at_block * BLOCK : (at_block + 1) * BLOCK, :] = block
                at_block += 1
        core, own_y, own_x = place_ref[0], place_ref[1], place_ref[2]
        pieces = 2 * pieces_y * pieces_x
        size = packed.shape[0] // pieces
        half = pieces // 2
        for side, out_ref in ((0, keep_ref), (1, send_ref)):
            for slot in range(half):
                y = lax.rem(own_y + slot // pieces_x, pieces_y)
                x = lax.rem(own_x + slot % pieces_x, pieces_x)
                c = core if side == 0 else 1 - core
                piece = (c * pieces_y + y) * pieces_x + x
                out_ref[slot * size : (slot + 1) * size, :] = packed[
                    pl.ds(pl.multiple_of(piece * size, 8), size), :
                ]


def total(terms):
    while len(terms) > 1:
        terms = [terms[i] + terms[i + 1] if i + 1 < len(terms) else terms[i] for i in range(0, len(terms), 2)]
    return terms[0]


def invert_diagonal(work, base):
    tiles = BLOCK // 8
    lane = lax.broadcasted_iota(jnp.int32, (8, BLOCK), 1)
    sub = lax.broadcasted_iota(jnp.int32, (8, BLOCK), 0)
    rows = [work[pl.ds(base + 8 * t, 8), pl.ds(base, BLOCK)] for t in range(tiles)]
    for t in range(tiles):
        at = 8 * t
        mine = rows[t]
        current = [
            [jnp.broadcast_to(mine[i : i + 1, at + j : at + j + 1], (8, BLOCK)) for j in range(i + 1)]
            for i in range(8)
        ]
        outside = {
            s: [jnp.broadcast_to(rows[s][:, at + j : at + j + 1], (8, BLOCK)) for j in range(8)]
            for s in range(t + 1, tiles)
        }
        clear = (lane >= at) & (lane < at + 8)
        base_row = jnp.where(clear, jnp.where(lane - at == sub, 1.0, 0.0), mine)
        done = [jnp.broadcast_to(base_row[k : k + 1, :], (8, BLOCK)) for k in range(8)]
        pivots = []
        inv = [[None] * 8 for _ in range(8)]
        for k in range(8):
            recip = 1.0 / current[k][k]
            pivots.append(recip)
            for i in range(k + 1, 8):
                for j in range(k + 1, i + 1):
                    current[i][j] = current[i][j] - (current[i][k] * current[j][k]) * recip
            for i in range(k + 1, 8):
                unit = current[i][k] * recip
                done[i] = done[i] - unit * done[k]
                for j in range(k):
                    inv[i][j] = inv[i][j] - unit * inv[k][j]
                inv[i][k] = -unit
        scaled = [done[i] * pivots[i] for i in range(8)]
        solved = [total([scaled[j]] + [inv[i][j] * scaled[i] for i in range(j + 1, 8)]) for j in range(8)]
        for s in range(t + 1, tiles):
            left = jnp.where(clear, 0.0, rows[s])
            rows[s] = left - total([outside[s][j] * solved[j] for j in range(8)])
        out = done[0] * lax.rsqrt(current[0][0])
        for i in range(1, 8):
            out = jnp.where(sub == i, done[i] * lax.rsqrt(current[i][i]), out)
        rows[t] = jnp.where(lane < at + 8, out, 0.0)
    return rows


def factor_body(sizes, place_ref, parts_ref, inverse_ref, scale_ref, packed, corner, full):
    pieces_y, pieces_x, obs_total, members = sizes
    core, own_y, own_x = place_ref[0], place_ref[1], place_ref[2]
    pieces = 2 * pieces_y * pieces_x
    size = packed.shape[0] // pieces
    half = pieces // 2
    for side in range(2):
        for slot in range(half):
            y = lax.rem(own_y + slot // pieces_x, pieces_y)
            x = lax.rem(own_x + slot % pieces_x, pieces_x)
            c = core if side == 0 else 1 - core
            piece = (c * pieces_y + y) * pieces_x + x
            packed[pl.ds(pl.multiple_of(piece * size, 8), size), :] = parts_ref[
                (side * half + slot) * size : (side * half + slot + 1) * size, :
            ].astype(F32)
    count = full.shape[0]
    blocks = count // BLOCK
    row_at = lax.broadcasted_iota(jnp.int32, (BLOCK, BLOCK), 0)
    lane_at = lax.broadcasted_iota(jnp.int32, (BLOCK, BLOCK), 1)
    square_sum = packed[2:3, SLOT : SLOT + 1]
    prior_scale = 2.0 / (1.0 + square_sum / obs_total)
    gains = []
    at_block = 0
    for i in range(blocks):
        for j in range(i + 1):
            block = packed[at_block * BLOCK : (at_block + 1) * BLOCK, :]
            at_block += 1
            if i == j:
                first = pltpu.roll(jnp.broadcast_to(block[0:1], (8, BLOCK)), SLOT, axis=1)[0:1]
                gains.append(jnp.where(lane_at[0:1] < SLOT, first, block[1:2]))
                block = jnp.where(row_at >= lane_at, block, block.T)
                block = block * prior_scale + jnp.where(row_at == lane_at, 1.0, 0.0)
                full[i * BLOCK : (i + 1) * BLOCK, j * BLOCK : (j + 1) * BLOCK] = block
            else:
                block = block * prior_scale
                full[i * BLOCK : (i + 1) * BLOCK, j * BLOCK : (j + 1) * BLOCK] = block
                full[j * BLOCK : (j + 1) * BLOCK, i * BLOCK : (i + 1) * BLOCK] = block.T
    def eliminate(b):
        low, high = b * BLOCK, (b + 1) * BLOCK
        diag = corner[...]
        if b > 0:
            left = jnp.dot(diag, full[low:high, :low], precision=HIGHEST, preferred_element_type=F32)
        if high < count:
            right = jnp.dot(diag, full[low:high, high:], precision=HIGHEST, preferred_element_type=F32)
            for i in range(b + 1, blocks):
                ilow, ihigh = i * BLOCK, (i + 1) * BLOCK
                factor = right[:, ilow - high : ihigh - high]
                full[ilow:ihigh, high:] = full[ilow:ihigh, high:] - lax.dot_general(
                    factor, right, TN, precision=HIGHEST, preferred_element_type=F32
                )
                if b > 0:
                    full[ilow:ihigh, :low] = full[ilow:ihigh, :low] - lax.dot_general(
                        factor, left, TN, precision=HIGHEST, preferred_element_type=F32
                    )
                full[ilow:ihigh, low:high] = -lax.dot_general(
                    factor, diag, TN, precision=HIGHEST, preferred_element_type=F32
                )
            full[low:high, high:] = jnp.zeros((BLOCK, count - high), F32)
        full[low:high, low:high] = diag
        if b > 0:
            full[low:high, :low] = left

    def advance(b, carry):
        rows = invert_diagonal(full, pl.multiple_of(b * BLOCK, BLOCK))
        for t, row in enumerate(rows):
            corner[8 * t : 8 * t + 8, :] = row
        for k in range(blocks):
            pl.when(b == k)(lambda k=k: eliminate(k))
        return carry

    lax.fori_loop(0, blocks, advance, 0)
    inverse = full[...]
    gain = jnp.broadcast_to(jnp.concatenate(gains, axis=1), (8, count))
    inner = lax.dot_general(gain, inverse, NT, precision=HIGHEST, preferred_element_type=F32)
    weights = jnp.dot(inner, inverse, precision=HIGHEST, preferred_element_type=F32)
    weights = weights * jnp.sqrt(prior_scale)
    own_rows = inverse_ref.shape[0] - 16
    inverse_ref[:own_rows, :] = full[pl.ds(pl.multiple_of(own_y * own_rows, 8), own_rows), :].astype(BF16)
    inverse_ref[own_rows:, :] = jnp.broadcast_to(weights[0:1], (16, count)).astype(BF16)
    scale_ref[...] = jnp.broadcast_to(prior_scale, scale_ref.shape)


def apply_body(sizes, scale_ref, inverse_ref, table_ref, analysis_ref, increment_ref, columns):
    members, modes, lon_cols, inv_root = sizes
    own_rows = analysis_ref.shape[0]
    prior_scale = scale_ref[0:1, 0:1]
    analysis_scale = jnp.sqrt(prior_scale * (members - 1)) * inv_root
    increment_scale = jnp.sqrt(prior_scale) * inv_root
    for j in range(lon_cols):
        base = j * (members + modes)
        own = table_ref[base : base + members, :]
        picked = table_ref[base + members : base + members + modes, :]
        for mode in range(modes):
            columns[mode * members : (mode + 1) * members, :] = picked[mode : mode + 1] * own
        product = jnp.dot(inverse_ref[...], columns[...], preferred_element_type=F32)
        analysis_ref[:, j, :] = (product[:own_rows] * analysis_scale).astype(BF16)
        increment_ref[j : j + 1, :] = product[own_rows : own_rows + 1] * increment_scale


def local(perturb, eig_table, mode_index, mean_state, obs_col, obs_row, obs_frac, obs_value, obs_sigma):
    members, lon_cols, lat = perturb.shape
    table_rows = eig_table.shape[0]
    modes = mode_index.shape[0]
    obs_local = obs_col.shape[0]
    lon_devices = lax.axis_size("lon")
    ens_devices = lax.axis_size("ens")
    obs_total = obs_local * lon_devices
    count = modes * members
    obs_own = obs_local // ens_devices
    own_y = lax.axis_index("ens")
    lon = lax.axis_index("lon")
    xs = 4
    zs = lon_devices // (2 * xs)
    core = lon % 2
    own_x = lon // (2 * zs)
    place = jnp.stack([core, own_y, own_x]).astype(jnp.int32)
    inv_root = 1.0 / float(members - 1) ** 0.5
    obs_scale = (4.0 * members / obs_total) ** 0.5

    slot = members + modes
    cells = 512
    edge_rows = slot + 8
    edge = pl.pallas_call(
        edge_body,
        grid=(lat // 1024,),
        out_shape=jax.ShapeDtypeStruct((edge_rows, lat), BF16),
        in_specs=[
            smem(),
            pl.BlockSpec((members, lon_cols, 1024), lambda g: (0, 0, g)),
            pl.BlockSpec((table_rows, lon_cols, 1024), lambda g: (0, 0, g)),
            pl.BlockSpec((lon_cols, 1024), lambda g: (0, g)),
        ],
        out_specs=pl.BlockSpec((edge_rows, 1024), lambda g: (0, g)),
        scratch_shapes=[VMEM((modes, lon_cols, 1024), BF16)],
        name="edge",
    )(mode_index, perturb, eig_table, mean_state)
    back = [(source, (source - 1) % lon_devices) for source in range(lon_devices)]
    edge = lax.ppermute(edge, "lon", back)
    table = pl.pallas_call(
        table_body,
        grid=(lat // cells,),
        out_shape=jax.ShapeDtypeStruct((lon_cols * slot, lat), BF16),
        in_specs=[
            smem(),
            pl.BlockSpec((members, lon_cols, cells), lambda g: (0, 0, g)),
            pl.BlockSpec((table_rows, lon_cols, cells), lambda g: (0, 0, g)),
        ],
        out_specs=pl.BlockSpec((lon_cols * slot, cells), lambda g: (0, g)),
        scratch_shapes=[VMEM((modes, lon_cols, cells), BF16)],
        name="table",
    )(mode_index, perturb, eig_table)
    width = 256
    steps = obs_own // width
    blocks = count // BLOCK
    packed_rows = blocks * (blocks + 1) // 2 * BLOCK
    half = packed_rows // 2
    ys = ens_devices
    keep, send = pl.pallas_call(
        lambda *refs: observe_body((members, modes, obs_scale * inv_root, width, ys, xs), *refs),
        grid=(steps,),
        out_shape=[jax.ShapeDtypeStruct((half, BLOCK), F32)] * 2,
        in_specs=[smem()] + [vmem()] * 8,
        out_specs=[vmem(), vmem()],
        scratch_shapes=[
            VMEM(((lon_cols + 1) * slot + 16, lat), BF16),
            VMEM((count + 16, obs_own), BF16),
            VMEM((packed_rows, BLOCK), F32),
        ],
        name="observe",
    )(
        place,
        *[v.reshape(1, obs_local) for v in (obs_col, obs_row, obs_frac, obs_value, obs_sigma)],
        table,
        edge,
        mean_state,
    )

    def at(x, z, c):
        return ((x % xs) * zs + z % zs) * 2 + c

    spots = [(x, z, c) for x in range(xs) for z in range(zs) for c in range(2)]
    over_core = [(at(x, z, c), at(x, z, 1 - c)) for x, z, c in spots]

    def over_x(d):
        return [(at(x, z, c), at(x + d, z, c)) for x, z, c in spots]

    def over_z(d):
        return [(at(x, z, c), at(x, z ^ d, c)) for x, z, c in spots]

    def over_y(d):
        return [(y, (y + d) % ys) for y in range(ys)]

    quarter = half // ys
    piece = quarter // xs
    got = lax.ppermute(send, "lon", over_core)
    mine = keep + got
    got = [lax.ppermute(mine[d * quarter : (d + 1) * quarter], "ens", over_y(d)) for d in range(1, ys)]
    mine = mine[:quarter] + sum(got)
    got = [lax.ppermute(mine[d * piece : (d + 1) * piece], "lon", over_x(d)) for d in range(1, xs)]
    mine = mine[:piece] + sum(got)
    d = 1
    while d < zs:
        mine = mine + lax.ppermute(mine, "lon", over_z(d))
        d *= 2
    got = [lax.ppermute(mine, "lon", over_x(-d)) for d in range(1, xs)]
    mine = jnp.concatenate([mine] + got)
    got = [lax.ppermute(mine, "ens", over_y(-d)) for d in range(1, ys)]
    mine = jnp.concatenate([mine] + got)
    got = lax.ppermute(mine, "lon", over_core)
    parts = jnp.concatenate([mine, got])

    own_columns = count // ens_devices
    inverse, scale = pl.pallas_call(
        lambda *refs: factor_body((ys, xs, float(obs_total), members), *refs),
        out_shape=[
            jax.ShapeDtypeStruct((own_columns + 16, count), BF16),
            jax.ShapeDtypeStruct((8, 128), F32),
        ],
        in_specs=[smem(), vmem()],
        out_specs=[vmem(), vmem()],
        scratch_shapes=[VMEM((packed_rows, BLOCK), F32), VMEM((BLOCK, BLOCK), F32), VMEM((count, count), F32)],
        name="factor",
    )(place, parts)
    analysis, increment = pl.pallas_call(
        lambda *refs: apply_body((members, modes, lon_cols, inv_root), *refs),
        grid=(lat // cells,),
        out_shape=[
            jax.ShapeDtypeStruct((own_columns, lon_cols, lat), BF16),
            jax.ShapeDtypeStruct((lon_cols, lat), F32),
        ],
        in_specs=[
            vmem(),
            vmem(),
            pl.BlockSpec((lon_cols * slot, cells), lambda g: (0, g)),
        ],
        out_specs=[
            pl.BlockSpec((own_columns, lon_cols, cells), lambda g: (0, 0, g)),
            pl.BlockSpec((lon_cols, cells), lambda g: (0, g)),
        ],
        scratch_shapes=[VMEM((count, cells), BF16)],
        name="apply",
    )(scale, inverse, table)
    return (analysis, increment)


def solution(mesh):
    return jax.shard_map(
        local,
        mesh=mesh,
        in_specs=(
            P(None, "lon", None),
            P(None, "lon", None),
            P(),
            P("lon", None),
            P("lon"),
            P("lon"),
            P("lon"),
            P("lon"),
            P("lon"),
        ),
        out_specs=(P("ens", "lon", None), P("lon", None)),
        check_vma=False,
    )
```

```python
import jax
import jax.numpy as jnp
from jax import lax
from jax.experimental import pallas as pl
from jax.experimental.pallas import tpu as pltpu
from jax.sharding import PartitionSpec as P


F32 = jnp.float32
BF16 = jnp.bfloat16
HIGHEST = lax.Precision.HIGHEST
SMEM = pltpu.SMEM
VMEM = pltpu.VMEM

BLOCK = 128
SLOT = 64
NT = (((1,), (1,)), ((), ()))
TN = (((0,), (0,)), ((), ()))


def vmem(*shape_dtype):
    return pl.BlockSpec(memory_space=VMEM)


def smem():
    return pl.BlockSpec(memory_space=SMEM)


def position(pieces_x):
    lon = lax.axis_index("lon")
    return lon % 2, lax.axis_index("ens"), lon // (lax.axis_size("lon") // pieces_x)


def widen(index_ref, pert_ref, eig_ref, wide, lane):
    members, lon_cols, _ = pert_ref.shape
    cut = slice(lane * 128, (lane + 1) * 128)
    for member in range(members):
        wide[lane, member * lon_cols : (member + 1) * lon_cols, :] = pert_ref[member, :, cut].astype(F32)
    for mode in range(index_ref.shape[0]):
        at = (members + mode) * lon_cols
        wide[lane, at : at + lon_cols, :] = eig_ref[index_ref[mode], :, cut].astype(F32)
    return cut


def edge_body(index_ref, pert_ref, eig_ref, mean_ref, edge_ref, wide):
    members, lon_cols, lat = pert_ref.shape
    slot = members + index_ref.shape[0]
    for lane in range(lat // 128):
        cut = widen(index_ref, pert_ref, eig_ref, wide, lane)
        edge_ref[:slot, cut] = wide[lane, pl.ds(0, slot, stride=lon_cols), :].astype(BF16)
    rest = edge_ref.shape[0] - slot
    mean_row = mean_ref[0:1, :].astype(F32)
    edge_ref[slot:, :] = jnp.broadcast_to(mean_row, (rest, lat)).astype(BF16)


def table_body(index_ref, pert_ref, eig_ref, table_ref, wide):
    members, lon_cols, lat = pert_ref.shape
    slot = members + index_ref.shape[0]
    for lane in range(lat // 128):
        cut = widen(index_ref, pert_ref, eig_ref, wide, lane)
        for j in range(lon_cols):
            table_ref[j * slot : (j + 1) * slot, cut] = wide[
                lane, pl.ds(j, slot, stride=lon_cols), :
            ].astype(BF16)


def observe_body(
    sizes, col_ref, row_ref, frac_ref, value_ref, sigma_ref, table_ref, edge_ref, mean_ref,
    keep_ref, send_ref, cells, columns, packed,
):
    members, modes, obs_scale_root, width, pieces_y, pieces_x = sizes
    step = pl.program_id(0)
    steps = pl.num_programs(0)
    lon_cols, lat = mean_ref.shape
    slot = members + modes
    count = members * modes
    mean_at = (lon_cols + 1) * slot

    @pl.when(step == 0)
    def _():
        cells[: lon_cols * slot, :] = table_ref[...]
        cells[lon_cols * slot : mean_at, :] = edge_ref[:slot, :]
        rest = cells.shape[0] - mean_at
        line = lax.broadcasted_iota(jnp.int32, (rest, lat), 0)
        means = jnp.zeros((rest, lat), F32)
        for j in range(lon_cols):
            means = jnp.where(line == j, mean_ref[j : j + 1, :].astype(F32), means)
        means = jnp.where(line == lon_cols, edge_ref[slot : slot + 1, :].astype(F32), means)
        cells[mean_at:, :] = means.astype(BF16)

    at = pl.multiple_of((lax.axis_index("ens") * steps + step) * width, 128)
    col = col_ref[:, pl.ds(at, width)]
    row = row_ref[:, pl.ds(at, width)]
    fraction = frac_ref[:, pl.ds(at, width)]
    observed = value_ref[:, pl.ds(at, width)]
    obs_error = sigma_ref[:, pl.ds(at, width)]
    high = row // 256
    low = row - high * 256
    spread_high = jnp.broadcast_to(high, (16, width))
    spread_low = jnp.broadcast_to(low, (16, width))
    place = lax.broadcasted_iota(jnp.int32, (256, width), 0).astype(F32).astype(BF16)
    one = jnp.ones((256, width), BF16)
    none = jnp.zeros((256, width), BF16)
    chunk = 4
    found = None
    for start in range(0, lat // 256, chunk):
        parts = []
        for part in range(start, start + chunk):
            wanted = jnp.where(spread_high == part, spread_low, -1).astype(F32).astype(BF16)
            parts.append(jnp.where(place == jnp.concatenate([wanted] * 16, axis=0), one, none))
        hot = jnp.concatenate(parts, axis=0)
        piece = jnp.dot(
            cells[:, start * 256 : (start + chunk) * 256], hot, preferred_element_type=F32
        )
        found = piece if found is None else found + piece
    here = found[:slot]
    beyond = found[slot : 2 * slot]
    mean_here = found[mean_at : mean_at + 1]
    mean_next = found[mean_at + 1 : mean_at + 2]
    for j in range(1, lon_cols):
        pick = col == j
        here = jnp.where(pick, found[j * slot : (j + 1) * slot], here)
        beyond = jnp.where(pick, found[(j + 1) * slot : (j + 2) * slot], beyond)
        mean_here = jnp.where(pick, found[mean_at + j : mean_at + j + 1], mean_here)
        mean_next = jnp.where(pick, found[mean_at + j + 1 : mean_at + j + 2], mean_next)
    weight = obs_scale_root / obs_error
    pert_here = here[:members]
    pert_next = beyond[:members]
    mode_here = here[members:] * ((1.0 - fraction) * weight)
    mode_next = beyond[members:] * (fraction * weight)
    normed = (observed - ((1.0 - fraction) * mean_here + fraction * mean_next)) / obs_error
    own = pl.multiple_of(step * width, 128)
    for mode in range(modes):
        block = mode_here[mode : mode + 1] * pert_here + mode_next[mode : mode + 1] * pert_next
        columns[mode * members : (mode + 1) * members, pl.ds(own, width)] = block.astype(BF16)
    normed_high = normed.astype(BF16).astype(F32)
    normed_low = normed - normed_high
    which = lax.broadcasted_iota(jnp.int32, (16, width), 0)
    extra = jnp.where(
        which == 0,
        jnp.broadcast_to(normed_high, (16, width)),
        jnp.where(which == 1, jnp.broadcast_to(normed_low, (16, width)), 0.0),
    )
    columns[count : count + 16, pl.ds(own, width)] = extra.astype(BF16)

    @pl.when(step == steps - 1)
    def _():
        everything = columns[...]
        blocks = count // BLOCK
        tail = lax.dot_general(
            everything[count:], everything, NT, preferred_element_type=F32
        )
        gain = tail[0:1, :count] + tail[1:2, :count]
        own = everything[count:].astype(F32)
        total_normed = own[0:1] + own[1:2]
        square_sum = jnp.sum(total_normed * total_normed)
        row_at = lax.broadcasted_iota(jnp.int32, (BLOCK, BLOCK), 0)
        lane_at = lax.broadcasted_iota(jnp.int32, (BLOCK, BLOCK), 1)
        at_block = 0
        for i in range(blocks):
            strip = lax.dot_general(
                everything[i * BLOCK : (i + 1) * BLOCK],
                everything[: (i + 1) * BLOCK],
                NT,
                preferred_element_type=F32,
            )
            for j in range(i + 1):
                block = strip[:, j * BLOCK : (j + 1) * BLOCK]
                if i == j:
                    part = gain[:, i * BLOCK : (i + 1) * BLOCK]
                    turned = pltpu.roll(jnp.broadcast_to(part, (8, BLOCK)), SLOT, axis=1)
                    upper = lane_at >= SLOT
                    block = jnp.where((row_at == 0) & upper, jnp.broadcast_to(turned[0:1], (BLOCK, BLOCK)), block)
                    block = jnp.where(
                        (row_at == 1) & upper, jnp.broadcast_to(part, (BLOCK, BLOCK)), block
                    )
                    if i == 0:
                        block = jnp.where((row_at == 2) & upper, square_sum, block)
                packed[at_block * BLOCK : (at_block + 1) * BLOCK, :] = block
                at_block += 1
        core, own_y, own_x = position(pieces_x)
        pieces = 2 * pieces_y * pieces_x
        size = packed.shape[0] // pieces
        half = pieces // 2
        for side, out_ref in ((0, keep_ref), (1, send_ref)):
            for slot in range(half):
                y = lax.rem(own_y + slot // pieces_x, pieces_y)
                x = lax.rem(own_x + slot % pieces_x, pieces_x)
                c = core if side == 0 else 1 - core
                piece = (c * pieces_y + y) * pieces_x + x
                out_ref[slot * size : (slot + 1) * size, :] = packed[
                    pl.ds(pl.multiple_of(piece * size, 8), size), :
                ]


def total(terms):
    while len(terms) > 1:
        terms = [terms[i] + terms[i + 1] if i + 1 < len(terms) else terms[i] for i in range(0, len(terms), 2)]
    return terms[0]


def invert_diagonal(work, base):
    tiles = BLOCK // 8
    lane = lax.broadcasted_iota(jnp.int32, (8, BLOCK), 1)
    sub = lax.broadcasted_iota(jnp.int32, (8, BLOCK), 0)
    rows = [work[pl.ds(base + 8 * t, 8), pl.ds(base, BLOCK)] for t in range(tiles)]
    for t in range(tiles):
        at = 8 * t
        mine = rows[t]
        current = [
            [jnp.broadcast_to(mine[i : i + 1, at + j : at + j + 1], (8, BLOCK)) for j in range(i + 1)]
            for i in range(8)
        ]
        outside = {
            s: [jnp.broadcast_to(rows[s][:, at + j : at + j + 1], (8, BLOCK)) for j in range(8)]
            for s in range(t + 1, tiles)
        }
        clear = (lane >= at) & (lane < at + 8)
        base_row = jnp.where(clear, jnp.where(lane - at == sub, 1.0, 0.0), mine)
        done = [jnp.broadcast_to(base_row[k : k + 1, :], (8, BLOCK)) for k in range(8)]
        pivots = []
        roots = []
        inv = [[None] * 8 for _ in range(8)]
        for k in range(0, 8, 2):
            first, cross, second = current[k][k], current[k + 1][k], current[k + 1][k + 1]
            det = first * second - cross * cross
            recip = 1.0 / first
            recip_det = 1.0 / det
            pivots += [recip, first * recip_det]
            roots += [first, det * recip]
            both = recip * recip_det
            turned = {i: first * current[i][k + 1] - cross * current[i][k] for i in range(k + 2, 8)}
            for i in range(k + 2, 8):
                for j in range(k + 2, i + 1):
                    value = current[i][j] - (current[i][k] * current[j][k]) * recip
                    current[i][j] = value - (turned[i] * turned[j]) * both
            for kk in (k, k + 1):
                for i in range(kk + 1, 8):
                    if kk > k:
                        unit = turned[i] * recip_det
                    else:
                        unit = current[i][k] * recip
                    done[i] = done[i] - unit * done[kk]
                    for j in range(kk):
                        inv[i][j] = inv[i][j] - unit * inv[kk][j]
                    inv[i][kk] = -unit
        scaled = [done[i] * pivots[i] for i in range(8)]
        solved = [total([scaled[j]] + [inv[i][j] * scaled[i] for i in range(j + 1, 8)]) for j in range(8)]
        for s in range(t + 1, tiles):
            left = jnp.where(clear, 0.0, rows[s])
            rows[s] = left - total([outside[s][j] * solved[j] for j in range(8)])
        out = done[0] * lax.rsqrt(roots[0])
        for i in range(1, 8):
            out = jnp.where(sub == i, done[i] * lax.rsqrt(roots[i]), out)
        rows[t] = jnp.where(lane < at + 8, out, 0.0)
    return rows


def factor_body(sizes, parts_ref, inverse_ref, scale_ref, packed, corner, full):
    pieces_y, pieces_x, obs_total, members = sizes
    core, own_y, own_x = position(pieces_x)
    pieces = 2 * pieces_y * pieces_x
    size = packed.shape[0] // pieces
    half = pieces // 2
    for side in range(2):
        for slot in range(half):
            y = lax.rem(own_y + slot // pieces_x, pieces_y)
            x = lax.rem(own_x + slot % pieces_x, pieces_x)
            c = core if side == 0 else 1 - core
            piece = (c * pieces_y + y) * pieces_x + x
            packed[pl.ds(pl.multiple_of(piece * size, 8), size), :] = parts_ref[
                (side * half + slot) * size : (side * half + slot + 1) * size, :
            ].astype(F32)
    count = full.shape[0]
    blocks = count // BLOCK
    row_at = lax.broadcasted_iota(jnp.int32, (BLOCK, BLOCK), 0)
    lane_at = lax.broadcasted_iota(jnp.int32, (BLOCK, BLOCK), 1)
    square_sum = packed[2:3, SLOT : SLOT + 1]
    prior_scale = 2.0 / (1.0 + square_sum / obs_total)
    gains = []
    at_block = 0
    for i in range(blocks):
        for j in range(i + 1):
            block = packed[at_block * BLOCK : (at_block + 1) * BLOCK, :]
            at_block += 1
            if i == j:
                first = pltpu.roll(jnp.broadcast_to(block[0:1], (8, BLOCK)), SLOT, axis=1)[0:1]
                gains.append(jnp.where(lane_at[0:1] < SLOT, first, block[1:2]))
                block = jnp.where(row_at >= lane_at, block, block.T)
                block = block * prior_scale + jnp.where(row_at == lane_at, 1.0, 0.0)
                full[i * BLOCK : (i + 1) * BLOCK, j * BLOCK : (j + 1) * BLOCK] = block
            else:
                block = block * prior_scale
                full[i * BLOCK : (i + 1) * BLOCK, j * BLOCK : (j + 1) * BLOCK] = block
                full[j * BLOCK : (j + 1) * BLOCK, i * BLOCK : (i + 1) * BLOCK] = block.T
    def eliminate(b):
        low, high = b * BLOCK, (b + 1) * BLOCK
        diag = corner[...]
        if b > 0:
            left = jnp.dot(diag, full[low:high, :low], precision=HIGHEST, preferred_element_type=F32)
        if high < count:
            right = jnp.dot(diag, full[low:high, high:], precision=HIGHEST, preferred_element_type=F32)
            for i in range(b + 1, blocks):
                ilow, ihigh = i * BLOCK, (i + 1) * BLOCK
                factor = right[:, ilow - high : ihigh - high]
                full[ilow:ihigh, high:] = full[ilow:ihigh, high:] - lax.dot_general(
                    factor, right, TN, precision=HIGHEST, preferred_element_type=F32
                )
                if b > 0:
                    full[ilow:ihigh, :low] = full[ilow:ihigh, :low] - lax.dot_general(
                        factor, left, TN, precision=HIGHEST, preferred_element_type=F32
                    )
                full[ilow:ihigh, low:high] = -lax.dot_general(
                    factor, diag, TN, precision=HIGHEST, preferred_element_type=F32
                )
            full[low:high, high:] = jnp.zeros((BLOCK, count - high), F32)
        full[low:high, low:high] = diag
        if b > 0:
            full[low:high, :low] = left

    def advance(b, carry):
        rows = invert_diagonal(full, pl.multiple_of(b * BLOCK, BLOCK))
        for t, row in enumerate(rows):
            corner[8 * t : 8 * t + 8, :] = row
        for k in range(blocks):
            pl.when(b == k)(lambda k=k: eliminate(k))
        return carry

    lax.fori_loop(0, blocks, advance, 0)
    inverse = full[...]
    gain = jnp.broadcast_to(jnp.concatenate(gains, axis=1), (8, count))
    inner = lax.dot_general(gain, inverse, NT, precision=HIGHEST, preferred_element_type=F32)
    weights = jnp.dot(inner, inverse, precision=HIGHEST, preferred_element_type=F32)
    weights = weights * jnp.sqrt(prior_scale)
    own_rows = inverse_ref.shape[0] - 16
    inverse_ref[:own_rows, :] = full[pl.ds(pl.multiple_of(own_y * own_rows, 8), own_rows), :].astype(BF16)
    inverse_ref[own_rows:, :] = jnp.broadcast_to(weights[0:1], (16, count)).astype(BF16)
    scale_ref[...] = jnp.broadcast_to(prior_scale, scale_ref.shape)


def apply_body(sizes, scale_ref, inverse_ref, table_ref, analysis_ref, increment_ref, columns, wide):
    members, modes, lon_cols, inv_root = sizes
    own_rows = analysis_ref.shape[0]
    prior_scale = scale_ref[0:1, 0:1]
    analysis_scale = jnp.sqrt(prior_scale * (members - 1)) * inv_root
    increment_scale = jnp.sqrt(prior_scale) * inv_root
    for j in range(lon_cols):
        base = j * (members + modes)
        own = table_ref[base : base + members, :]
        picked = table_ref[base + members : base + members + modes, :]
        for mode in range(modes):
            columns[mode * members : (mode + 1) * members, :] = picked[mode : mode + 1] * own
        product = jnp.dot(inverse_ref[...], columns[...], preferred_element_type=F32)
        for lane in range(wide.shape[0]):
            cut = slice(lane * 128, (lane + 1) * 128)
            wide[lane, pl.ds(j, own_rows, stride=lon_cols), :] = product[:own_rows, cut] * analysis_scale
        increment_ref[j : j + 1, :] = product[own_rows : own_rows + 1] * increment_scale
    for lane in range(wide.shape[0]):
        cut = slice(lane * 128, (lane + 1) * 128)
        analysis_ref[:, :, cut] = wide[lane].astype(BF16).reshape(own_rows, lon_cols, 128)


def local(perturb, eig_table, mode_index, mean_state, obs_col, obs_row, obs_frac, obs_value, obs_sigma):
    members, lon_cols, lat = perturb.shape
    table_rows = eig_table.shape[0]
    modes = mode_index.shape[0]
    obs_local = obs_col.shape[0]
    lon_devices = lax.axis_size("lon")
    ens_devices = lax.axis_size("ens")
    obs_total = obs_local * lon_devices
    count = modes * members
    obs_own = obs_local // ens_devices
    xs = 4
    zs = lon_devices // (2 * xs)
    inv_root = 1.0 / float(members - 1) ** 0.5
    obs_scale = (4.0 * members / obs_total) ** 0.5

    slot = members + modes
    cells = 2048
    edge_rows = slot + 8
    edge = pl.pallas_call(
        edge_body,
        grid=(lat // cells,),
        out_shape=jax.ShapeDtypeStruct((edge_rows, lat), BF16),
        in_specs=[
            smem(),
            pl.BlockSpec((members, lon_cols, cells), lambda g: (0, 0, g)),
            pl.BlockSpec((table_rows, lon_cols, cells), lambda g: (0, 0, g)),
            pl.BlockSpec((lon_cols, cells), lambda g: (0, g)),
        ],
        out_specs=pl.BlockSpec((edge_rows, cells), lambda g: (0, g)),
        scratch_shapes=[VMEM((cells // 128, slot * lon_cols, 128), F32)],
        name="edge",
    )(mode_index, perturb, eig_table, mean_state)
    back = [(source, (source - 1) % lon_devices) for source in range(lon_devices)]
    edge = lax.ppermute(edge, "lon", back)
    table = pl.pallas_call(
        table_body,
        grid=(lat // cells,),
        out_shape=jax.ShapeDtypeStruct((lon_cols * slot, lat), BF16),
        in_specs=[
            smem(),
            pl.BlockSpec((members, lon_cols, cells), lambda g: (0, 0, g)),
            pl.BlockSpec((table_rows, lon_cols, cells), lambda g: (0, 0, g)),
        ],
        out_specs=pl.BlockSpec((lon_cols * slot, cells), lambda g: (0, g)),
        scratch_shapes=[VMEM((cells // 128, slot * lon_cols, 128), F32)],
        name="table",
    )(mode_index, perturb, eig_table)
    width = 256
    steps = obs_own // width
    blocks = count // BLOCK
    packed_rows = blocks * (blocks + 1) // 2 * BLOCK
    half = packed_rows // 2
    ys = ens_devices
    keep, send = pl.pallas_call(
        lambda *refs: observe_body((members, modes, obs_scale * inv_root, width, ys, xs), *refs),
        grid=(steps,),
        out_shape=[jax.ShapeDtypeStruct((half, BLOCK), F32)] * 2,
        in_specs=[vmem()] * 8,
        out_specs=[vmem(), vmem()],
        scratch_shapes=[
            VMEM(((lon_cols + 1) * slot + 16, lat), BF16),
            VMEM((count + 16, obs_own), BF16),
            VMEM((packed_rows, BLOCK), F32),
        ],
        name="observe",
    )(
        *[v.reshape(1, obs_local) for v in (obs_col, obs_row, obs_frac, obs_value, obs_sigma)],
        table,
        edge,
        mean_state,
    )

    def at(x, z, c):
        return ((x % xs) * zs + z % zs) * 2 + c

    spots = [(x, z, c) for x in range(xs) for z in range(zs) for c in range(2)]
    over_core = [(at(x, z, c), at(x, z, 1 - c)) for x, z, c in spots]

    def over_x(d):
        return [(at(x, z, c), at(x + d, z, c)) for x, z, c in spots]

    def over_z(d):
        return [(at(x, z, c), at(x, z ^ d, c)) for x, z, c in spots]

    def over_y(d):
        return [(y, (y + d) % ys) for y in range(ys)]

    quarter = half // ys
    piece = quarter // xs
    got = lax.ppermute(send, "lon", over_core)
    mine = keep + got
    got = [lax.ppermute(mine[d * quarter : (d + 1) * quarter], "ens", over_y(d)) for d in range(1, ys)]
    mine = mine[:quarter] + sum(got)
    got = [lax.ppermute(mine[d * piece : (d + 1) * piece], "lon", over_x(d)) for d in range(1, xs)]
    mine = mine[:piece] + sum(got)
    d = 1
    while d < zs:
        mine = mine + lax.ppermute(mine, "lon", over_z(d))
        d *= 2
    got = [lax.ppermute(mine, "lon", over_x(-d)) for d in range(1, xs)]
    mine = jnp.concatenate([mine] + got)
    got = [lax.ppermute(mine, "ens", over_y(-d)) for d in range(1, ys)]
    mine = jnp.concatenate([mine] + got)
    got = lax.ppermute(mine, "lon", over_core)
    parts = jnp.concatenate([mine, got])

    own_columns = count // ens_devices
    inverse, scale = pl.pallas_call(
        lambda *refs: factor_body((ys, xs, float(obs_total), members), *refs),
        out_shape=[
            jax.ShapeDtypeStruct((own_columns + 16, count), BF16),
            jax.ShapeDtypeStruct((8, 128), F32),
        ],
        in_specs=[vmem()],
        out_specs=[vmem(), vmem()],
        scratch_shapes=[VMEM((packed_rows, BLOCK), F32), VMEM((BLOCK, BLOCK), F32), VMEM((count, count), F32)],
        name="factor",
    )(parts)
    cells = 1024
    analysis, increment = pl.pallas_call(
        lambda *refs: apply_body((members, modes, lon_cols, inv_root), *refs),
        grid=(lat // cells,),
        out_shape=[
            jax.ShapeDtypeStruct((own_columns, lon_cols, lat), BF16),
            jax.ShapeDtypeStruct((lon_cols, lat), F32),
        ],
        in_specs=[
            vmem(),
            vmem(),
            pl.BlockSpec((lon_cols * slot, cells), lambda g: (0, g)),
        ],
        out_specs=[
            pl.BlockSpec((own_columns, lon_cols, cells), lambda g: (0, 0, g)),
            pl.BlockSpec((lon_cols, cells), lambda g: (0, g)),
        ],
        scratch_shapes=[VMEM((count, cells), BF16), VMEM((cells // 128, own_columns * lon_cols, 128), F32)],
        name="apply",
    )(scale, inverse, table)
    return (analysis, increment)


def solution(mesh):
    return jax.shard_map(
        local,
        mesh=mesh,
        in_specs=(
            P(None, "lon", None),
            P(None, "lon", None),
            P(),
            P("lon", None),
            P("lon"),
            P("lon"),
            P("lon"),
            P("lon"),
            P("lon"),
        ),
        out_specs=(P("ens", "lon", None), P("lon", None)),
        check_vma=False,
    )
```

```python
import jax
import jax.numpy as jnp
from jax import lax
from jax.experimental import pallas as pl
from jax.experimental.pallas import tpu as pltpu
from jax.sharding import PartitionSpec as P


F32 = jnp.float32
BF16 = jnp.bfloat16
HIGHEST = lax.Precision.HIGHEST
SMEM = pltpu.SMEM
VMEM = pltpu.VMEM

BLOCK = 128
SLOT = 64
NT = (((1,), (1,)), ((), ()))
TN = (((0,), (0,)), ((), ()))


def vmem(*shape_dtype):
    return pl.BlockSpec(memory_space=VMEM)


def smem():
    return pl.BlockSpec(memory_space=SMEM)


def position(pieces_x):
    lon = lax.axis_index("lon")
    return lon % 2, lax.axis_index("ens"), lon // (lax.axis_size("lon") // pieces_x)


def widen(index_ref, pert_ref, eig_ref, wide, lane):
    members, lon_cols, _ = pert_ref.shape
    cut = slice(lane * 128, (lane + 1) * 128)
    for member in range(members):
        wide[lane, member * lon_cols : (member + 1) * lon_cols, :] = pert_ref[member, :, cut].astype(F32)
    for mode in range(index_ref.shape[0]):
        at = (members + mode) * lon_cols
        wide[lane, at : at + lon_cols, :] = eig_ref[index_ref[mode], :, cut].astype(F32)
    return cut


def edge_body(index_ref, pert_ref, eig_ref, mean_ref, edge_ref, wide):
    members, lon_cols, lat = pert_ref.shape
    slot = members + index_ref.shape[0]
    for lane in range(lat // 128):
        cut = widen(index_ref, pert_ref, eig_ref, wide, lane)
        edge_ref[:slot, cut] = wide[lane, pl.ds(0, slot, stride=lon_cols), :].astype(BF16)
    rest = edge_ref.shape[0] - slot
    mean_row = mean_ref[0:1, :].astype(F32)
    edge_ref[slot:, :] = jnp.broadcast_to(mean_row, (rest, lat)).astype(BF16)


def table_body(index_ref, pert_ref, eig_ref, table_ref, wide):
    members, lon_cols, lat = pert_ref.shape
    slot = members + index_ref.shape[0]
    for lane in range(lat // 128):
        cut = widen(index_ref, pert_ref, eig_ref, wide, lane)
        for j in range(lon_cols):
            table_ref[j * slot : (j + 1) * slot, cut] = wide[
                lane, pl.ds(j, slot, stride=lon_cols), :
            ].astype(BF16)


def observe_body(
    sizes, col_ref, row_ref, frac_ref, value_ref, sigma_ref, table_ref, edge_ref, mean_ref,
    keep_ref, send_ref, cells, columns, packed,
):
    members, modes, obs_scale_root, width, pieces_y, pieces_x = sizes
    step = pl.program_id(0)
    steps = pl.num_programs(0)
    lon_cols, lat = mean_ref.shape
    slot = members + modes
    count = members * modes
    mean_at = (lon_cols + 1) * slot

    @pl.when(step == 0)
    def _():
        cells[: lon_cols * slot, :] = table_ref[...]
        cells[lon_cols * slot : mean_at, :] = edge_ref[:slot, :]
        rest = cells.shape[0] - mean_at
        line = lax.broadcasted_iota(jnp.int32, (rest, lat), 0)
        means = jnp.zeros((rest, lat), F32)
        for j in range(lon_cols):
            means = jnp.where(line == j, mean_ref[j : j + 1, :].astype(F32), means)
        means = jnp.where(line == lon_cols, edge_ref[slot : slot + 1, :].astype(F32), means)
        cells[mean_at:, :] = means.astype(BF16)

    at = pl.multiple_of((lax.axis_index("ens") * steps + step) * width, 128)
    col = col_ref[:, pl.ds(at, width)]
    row = row_ref[:, pl.ds(at, width)]
    fraction = frac_ref[:, pl.ds(at, width)]
    observed = value_ref[:, pl.ds(at, width)]
    obs_error = sigma_ref[:, pl.ds(at, width)]
    high = row // 256
    low = row - high * 256
    spread_high = jnp.broadcast_to(high, (16, width))
    spread_low = jnp.broadcast_to(low, (16, width))
    place = lax.broadcasted_iota(jnp.int32, (256, width), 0).astype(F32).astype(BF16)
    one = jnp.ones((256, width), BF16)
    none = jnp.zeros((256, width), BF16)
    chunk = 2
    found = None
    for start in range(0, lat // 256, chunk):
        parts = []
        for part in range(start, start + chunk):
            wanted = jnp.where(spread_high == part, spread_low, -1).astype(F32).astype(BF16)
            parts.append(jnp.where(place == jnp.concatenate([wanted] * 16, axis=0), one, none))
        hot = jnp.concatenate(parts, axis=0)
        piece = jnp.dot(
            cells[:, start * 256 : (start + chunk) * 256], hot, preferred_element_type=F32
        )
        found = piece if found is None else found + piece
    here = found[:slot]
    beyond = found[slot : 2 * slot]
    mean_here = found[mean_at : mean_at + 1]
    mean_next = found[mean_at + 1 : mean_at + 2]
    for j in range(1, lon_cols):
        pick = col == j
        here = jnp.where(pick, found[j * slot : (j + 1) * slot], here)
        beyond = jnp.where(pick, found[(j + 1) * slot : (j + 2) * slot], beyond)
        mean_here = jnp.where(pick, found[mean_at + j : mean_at + j + 1], mean_here)
        mean_next = jnp.where(pick, found[mean_at + j + 1 : mean_at + j + 2], mean_next)
    weight = obs_scale_root / obs_error
    pert_here = here[:members]
    pert_next = beyond[:members]
    mode_here = here[members:] * ((1.0 - fraction) * weight)
    mode_next = beyond[members:] * (fraction * weight)
    normed = (observed - ((1.0 - fraction) * mean_here + fraction * mean_next)) / obs_error
    own = pl.multiple_of(step * width, 128)
    for mode in range(modes):
        block = mode_here[mode : mode + 1] * pert_here + mode_next[mode : mode + 1] * pert_next
        columns[mode * members : (mode + 1) * members, pl.ds(own, width)] = block.astype(BF16)
    normed_high = normed.astype(BF16).astype(F32)
    normed_low = normed - normed_high
    which = lax.broadcasted_iota(jnp.int32, (16, width), 0)
    extra = jnp.where(
        which == 0,
        jnp.broadcast_to(normed_high, (16, width)),
        jnp.where(which == 1, jnp.broadcast_to(normed_low, (16, width)), 0.0),
    )
    columns[count : count + 16, pl.ds(own, width)] = extra.astype(BF16)

    @pl.when(step == steps - 1)
    def _():
        everything = columns[...]
        blocks = count // BLOCK
        tail = lax.dot_general(
            everything[count:], everything, NT, preferred_element_type=F32
        )
        gain = tail[0:1, :count] + tail[1:2, :count]
        own = everything[count:].astype(F32)
        total_normed = own[0:1] + own[1:2]
        square_sum = jnp.sum(total_normed * total_normed)
        row_at = lax.broadcasted_iota(jnp.int32, (BLOCK, BLOCK), 0)
        lane_at = lax.broadcasted_iota(jnp.int32, (BLOCK, BLOCK), 1)
        at_block = 0
        for i in range(blocks):
            strip = lax.dot_general(
                everything[i * BLOCK : (i + 1) * BLOCK],
                everything[: (i + 1) * BLOCK],
                NT,
                preferred_element_type=F32,
            )
            for j in range(i + 1):
                block = strip[:, j * BLOCK : (j + 1) * BLOCK]
                if i == j:
                    part = gain[:, i * BLOCK : (i + 1) * BLOCK]
                    turned = pltpu.roll(jnp.broadcast_to(part, (8, BLOCK)), SLOT, axis=1)
                    upper = lane_at >= SLOT
                    block = jnp.where((row_at == 0) & upper, jnp.broadcast_to(turned[0:1], (BLOCK, BLOCK)), block)
                    block = jnp.where(
                        (row_at == 1) & upper, jnp.broadcast_to(part, (BLOCK, BLOCK)), block
                    )
                    if i == 0:
                        block = jnp.where((row_at == 2) & upper, square_sum, block)
                packed[at_block * BLOCK : (at_block + 1) * BLOCK, :] = block
                at_block += 1
        core, own_y, own_x = position(pieces_x)
        pieces = 2 * pieces_y * pieces_x
        size = packed.shape[0] // pieces
        half = pieces // 2
        for side, out_ref in ((0, keep_ref), (1, send_ref)):
            for slot in range(half):
                y = own_y ^ (slot // pieces_x)
                x = own_x ^ (slot % pieces_x)
                c = core if side == 0 else 1 - core
                piece = (c * pieces_y + y) * pieces_x + x
                out_ref[slot * size : (slot + 1) * size, :] = packed[
                    pl.ds(pl.multiple_of(piece * size, 8), size), :
                ]


def total(terms):
    while len(terms) > 1:
        terms = [terms[i] + terms[i + 1] if i + 1 < len(terms) else terms[i] for i in range(0, len(terms), 2)]
    return terms[0]


def invert_diagonal(work, base):
    tiles = BLOCK // 8
    lane = lax.broadcasted_iota(jnp.int32, (8, BLOCK), 1)
    sub = lax.broadcasted_iota(jnp.int32, (8, BLOCK), 0)
    rows = [work[pl.ds(base + 8 * t, 8), pl.ds(base, BLOCK)] for t in range(tiles)]
    for t in range(tiles):
        at = 8 * t
        mine = rows[t]
        current = [
            [jnp.broadcast_to(mine[i : i + 1, at + j : at + j + 1], (8, BLOCK)) for j in range(i + 1)]
            for i in range(8)
        ]
        outside = {
            s: [jnp.broadcast_to(rows[s][:, at + j : at + j + 1], (8, BLOCK)) for j in range(8)]
            for s in range(t + 1, tiles)
        }
        clear = (lane >= at) & (lane < at + 8)
        base_row = jnp.where(clear, jnp.where(lane - at == sub, 1.0, 0.0), mine)
        done = [jnp.broadcast_to(base_row[k : k + 1, :], (8, BLOCK)) for k in range(8)]
        pivots = []
        roots = []
        inv = [[None] * 8 for _ in range(8)]
        for k in range(0, 8, 2):
            first, cross, second = current[k][k], current[k + 1][k], current[k + 1][k + 1]
            det = first * second - cross * cross
            recip = 1.0 / first
            recip_det = 1.0 / det
            pivots += [recip, first * recip_det]
            roots += [first, det * recip]
            both = recip * recip_det
            turned = {i: first * current[i][k + 1] - cross * current[i][k] for i in range(k + 2, 8)}
            for i in range(k + 2, 8):
                for j in range(k + 2, i + 1):
                    value = current[i][j] - (current[i][k] * current[j][k]) * recip
                    current[i][j] = value - (turned[i] * turned[j]) * both
            for kk in (k, k + 1):
                for i in range(kk + 1, 8):
                    if kk > k:
                        unit = turned[i] * recip_det
                    else:
                        unit = current[i][k] * recip
                    done[i] = done[i] - unit * done[kk]
                    for j in range(kk):
                        inv[i][j] = inv[i][j] - unit * inv[kk][j]
                    inv[i][kk] = -unit
        scaled = [done[i] * pivots[i] for i in range(8)]
        solved = [total([scaled[j]] + [inv[i][j] * scaled[i] for i in range(j + 1, 8)]) for j in range(8)]
        for s in range(t + 1, tiles):
            left = jnp.where(clear, 0.0, rows[s])
            rows[s] = left - total([outside[s][j] * solved[j] for j in range(8)])
        out = done[0] * lax.rsqrt(roots[0])
        for i in range(1, 8):
            out = jnp.where(sub == i, done[i] * lax.rsqrt(roots[i]), out)
        rows[t] = jnp.where(lane < at + 8, out, 0.0)
    return rows


def factor_body(sizes, parts_ref, inverse_ref, scale_ref, packed, corner, full):
    pieces_y, pieces_x, obs_total, members = sizes
    core, own_y, own_x = position(pieces_x)
    pieces = 2 * pieces_y * pieces_x
    size = packed.shape[0] // pieces
    half = pieces // 2
    for side in range(2):
        for slot in range(half):
            y = own_y ^ (slot // pieces_x)
            x = own_x ^ (slot % pieces_x)
            c = core if side == 0 else 1 - core
            piece = (c * pieces_y + y) * pieces_x + x
            packed[pl.ds(pl.multiple_of(piece * size, 8), size), :] = parts_ref[
                (side * half + slot) * size : (side * half + slot + 1) * size, :
            ].astype(F32)
    count = full.shape[0]
    blocks = count // BLOCK
    row_at = lax.broadcasted_iota(jnp.int32, (BLOCK, BLOCK), 0)
    lane_at = lax.broadcasted_iota(jnp.int32, (BLOCK, BLOCK), 1)
    square_sum = packed[2:3, SLOT : SLOT + 1]
    prior_scale = 2.0 / (1.0 + square_sum / obs_total)
    gains = []
    at_block = 0
    for i in range(blocks):
        for j in range(i + 1):
            block = packed[at_block * BLOCK : (at_block + 1) * BLOCK, :]
            at_block += 1
            if i == j:
                first = pltpu.roll(jnp.broadcast_to(block[0:1], (8, BLOCK)), SLOT, axis=1)[0:1]
                gains.append(jnp.where(lane_at[0:1] < SLOT, first, block[1:2]))
                block = jnp.where(row_at >= lane_at, block, block.T)
                block = block * prior_scale + jnp.where(row_at == lane_at, 1.0, 0.0)
                full[i * BLOCK : (i + 1) * BLOCK, j * BLOCK : (j + 1) * BLOCK] = block
            else:
                block = block * prior_scale
                full[i * BLOCK : (i + 1) * BLOCK, j * BLOCK : (j + 1) * BLOCK] = block
                full[j * BLOCK : (j + 1) * BLOCK, i * BLOCK : (i + 1) * BLOCK] = block.T
    def eliminate(b):
        low, high = b * BLOCK, (b + 1) * BLOCK
        diag = corner[...]
        if b > 0:
            left = jnp.dot(diag, full[low:high, :low], precision=HIGHEST, preferred_element_type=F32)
        if high < count:
            right = jnp.dot(diag, full[low:high, high:], precision=HIGHEST, preferred_element_type=F32)
            for i in range(b + 1, blocks):
                ilow, ihigh = i * BLOCK, (i + 1) * BLOCK
                factor = right[:, ilow - high : ihigh - high]
                full[ilow:ihigh, high:] = full[ilow:ihigh, high:] - lax.dot_general(
                    factor, right, TN, precision=HIGHEST, preferred_element_type=F32
                )
                if b > 0:
                    full[ilow:ihigh, :low] = full[ilow:ihigh, :low] - lax.dot_general(
                        factor, left, TN, precision=HIGHEST, preferred_element_type=F32
                    )
                full[ilow:ihigh, low:high] = -lax.dot_general(
                    factor, diag, TN, precision=HIGHEST, preferred_element_type=F32
                )
            full[low:high, high:] = jnp.zeros((BLOCK, count - high), F32)
        full[low:high, low:high] = diag
        if b > 0:
            full[low:high, :low] = left

    def advance(b, carry):
        rows = invert_diagonal(full, pl.multiple_of(b * BLOCK, BLOCK))
        for t, row in enumerate(rows):
            corner[8 * t : 8 * t + 8, :] = row
        for k in range(blocks):
            pl.when(b == k)(lambda k=k: eliminate(k))
        return carry

    lax.fori_loop(0, blocks, advance, 0)
    inverse = full[...]
    gain = jnp.broadcast_to(jnp.concatenate(gains, axis=1), (8, count))
    inner = lax.dot_general(gain, inverse, NT, precision=HIGHEST, preferred_element_type=F32)
    weights = jnp.dot(inner, inverse, precision=HIGHEST, preferred_element_type=F32)
    weights = weights * jnp.sqrt(prior_scale)
    own_rows = inverse_ref.shape[0] - 16
    inverse_ref[:own_rows, :] = full[pl.ds(pl.multiple_of(own_y * own_rows, 8), own_rows), :].astype(BF16)
    inverse_ref[own_rows:, :] = jnp.broadcast_to(weights[0:1], (16, count)).astype(BF16)
    scale_ref[...] = jnp.broadcast_to(prior_scale, scale_ref.shape)


def apply_body(sizes, scale_ref, inverse_ref, table_ref, analysis_ref, increment_ref, columns, wide):
    members, modes, lon_cols, inv_root = sizes
    own_rows = analysis_ref.shape[0]
    prior_scale = scale_ref[0:1, 0:1]
    analysis_scale = jnp.sqrt(prior_scale * (members - 1)) * inv_root
    increment_scale = jnp.sqrt(prior_scale) * inv_root
    for j in range(lon_cols):
        base = j * (members + modes)
        own = table_ref[base : base + members, :]
        picked = table_ref[base + members : base + members + modes, :]
        for mode in range(modes):
            columns[mode * members : (mode + 1) * members, :] = picked[mode : mode + 1] * own
        product = jnp.dot(inverse_ref[...], columns[...], preferred_element_type=F32)
        for lane in range(wide.shape[0]):
            cut = slice(lane * 128, (lane + 1) * 128)
            wide[lane, pl.ds(j, own_rows, stride=lon_cols), :] = product[:own_rows, cut] * analysis_scale
        increment_ref[j : j + 1, :] = product[own_rows : own_rows + 1] * increment_scale
    for lane in range(wide.shape[0]):
        cut = slice(lane * 128, (lane + 1) * 128)
        analysis_ref[:, :, cut] = wide[lane].astype(BF16).reshape(own_rows, lon_cols, 128)


def local(perturb, eig_table, mode_index, mean_state, obs_col, obs_row, obs_frac, obs_value, obs_sigma):
    members, lon_cols, lat = perturb.shape
    table_rows = eig_table.shape[0]
    modes = mode_index.shape[0]
    obs_local = obs_col.shape[0]
    lon_devices = lax.axis_size("lon")
    ens_devices = lax.axis_size("ens")
    obs_total = obs_local * lon_devices
    count = modes * members
    obs_own = obs_local // ens_devices
    xs = 4
    zs = lon_devices // (2 * xs)
    inv_root = 1.0 / float(members - 1) ** 0.5
    obs_scale = (4.0 * members / obs_total) ** 0.5

    slot = members + modes
    cells = 2048
    edge_rows = slot + 8
    edge = pl.pallas_call(
        edge_body,
        grid=(lat // cells,),
        out_shape=jax.ShapeDtypeStruct((edge_rows, lat), BF16),
        in_specs=[
            smem(),
            pl.BlockSpec((members, lon_cols, cells), lambda g: (0, 0, g)),
            pl.BlockSpec((table_rows, lon_cols, cells), lambda g: (0, 0, g)),
            pl.BlockSpec((lon_cols, cells), lambda g: (0, g)),
        ],
        out_specs=pl.BlockSpec((edge_rows, cells), lambda g: (0, g)),
        scratch_shapes=[VMEM((cells // 128, slot * lon_cols, 128), F32)],
        name="edge",
    )(mode_index, perturb, eig_table, mean_state)
    back = [(source, (source - 1) % lon_devices) for source in range(lon_devices)]
    edge = lax.ppermute(edge, "lon", back)
    table = pl.pallas_call(
        table_body,
        grid=(lat // cells,),
        out_shape=jax.ShapeDtypeStruct((lon_cols * slot, lat), BF16),
        in_specs=[
            smem(),
            pl.BlockSpec((members, lon_cols, cells), lambda g: (0, 0, g)),
            pl.BlockSpec((table_rows, lon_cols, cells), lambda g: (0, 0, g)),
        ],
        out_specs=pl.BlockSpec((lon_cols * slot, cells), lambda g: (0, g)),
        scratch_shapes=[VMEM((cells // 128, slot * lon_cols, 128), F32)],
        name="table",
    )(mode_index, perturb, eig_table)
    width = 1024
    steps = obs_own // width
    blocks = count // BLOCK
    packed_rows = blocks * (blocks + 1) // 2 * BLOCK
    half = packed_rows // 2
    ys = ens_devices
    keep, send = pl.pallas_call(
        lambda *refs: observe_body((members, modes, obs_scale * inv_root, width, ys, xs), *refs),
        grid=(steps,),
        out_shape=[jax.ShapeDtypeStruct((half, BLOCK), F32)] * 2,
        in_specs=[vmem()] * 8,
        out_specs=[vmem(), vmem()],
        scratch_shapes=[
            VMEM(((lon_cols + 1) * slot + 16, lat), BF16),
            VMEM((count + 16, obs_own), BF16),
            VMEM((packed_rows, BLOCK), F32),
        ],
        name="observe",
    )(
        *[v.reshape(1, obs_local) for v in (obs_col, obs_row, obs_frac, obs_value, obs_sigma)],
        table,
        edge,
        mean_state,
    )

    def at(x, z, c):
        return ((x % xs) * zs + z % zs) * 2 + c

    spots = [(x, z, c) for x in range(xs) for z in range(zs) for c in range(2)]
    over_core = [(at(x, z, c), at(x, z, 1 - c)) for x, z, c in spots]

    def over_x(d):
        return [(at(x, z, c), at(x ^ d, z, c)) for x, z, c in spots]

    def over_z(d):
        return [(at(x, z, c), at(x, z ^ d, c)) for x, z, c in spots]

    def over_y(d):
        return [(y, y ^ d) for y in range(ys)]

    quarter = half // ys
    piece = quarter // xs
    got = lax.ppermute(send, "lon", over_core)
    mine = keep + got
    got = [lax.ppermute(mine[d * quarter : (d + 1) * quarter], "ens", over_y(d)) for d in range(1, ys)]
    mine = mine[:quarter] + sum(got)
    got = [lax.ppermute(mine[d * piece : (d + 1) * piece], "lon", over_x(d)) for d in range(1, xs)]
    mine = mine[:piece] + sum(got)
    for d in (1, 2, 6):
        mine = mine + lax.ppermute(mine, "lon", over_z(d))
    got = [lax.ppermute(mine, "lon", over_x(d)) for d in range(1, xs)]
    mine = jnp.concatenate([mine] + got)
    got = [lax.ppermute(mine, "ens", over_y(d)) for d in range(1, ys)]
    mine = jnp.concatenate([mine] + got)
    got = lax.ppermute(mine, "lon", over_core)
    parts = jnp.concatenate([mine, got])

    own_columns = count // ens_devices
    inverse, scale = pl.pallas_call(
        lambda *refs: factor_body((ys, xs, float(obs_total), members), *refs),
        out_shape=[
            jax.ShapeDtypeStruct((own_columns + 16, count), BF16),
            jax.ShapeDtypeStruct((8, 128), F32),
        ],
        in_specs=[vmem()],
        out_specs=[vmem(), vmem()],
        scratch_shapes=[VMEM((packed_rows, BLOCK), F32), VMEM((BLOCK, BLOCK), F32), VMEM((count, count), F32)],
        name="factor",
    )(parts)
    cells = 1024
    analysis, increment = pl.pallas_call(
        lambda *refs: apply_body((members, modes, lon_cols, inv_root), *refs),
        grid=(lat // cells,),
        out_shape=[
            jax.ShapeDtypeStruct((own_columns, lon_cols, lat), BF16),
            jax.ShapeDtypeStruct((lon_cols, lat), F32),
        ],
        in_specs=[
            vmem(),
            vmem(),
            pl.BlockSpec((lon_cols * slot, cells), lambda g: (0, g)),
        ],
        out_specs=[
            pl.BlockSpec((own_columns, lon_cols, cells), lambda g: (0, 0, g)),
            pl.BlockSpec((lon_cols, cells), lambda g: (0, g)),
        ],
        scratch_shapes=[VMEM((count, cells), BF16), VMEM((cells // 128, own_columns * lon_cols, 128), F32)],
        name="apply",
    )(scale, inverse, table)
    return (analysis, increment)


def solution(mesh):
    return jax.shard_map(
        local,
        mesh=mesh,
        in_specs=(
            P(None, "lon", None),
            P(None, "lon", None),
            P(),
            P("lon", None),
            P("lon"),
            P("lon"),
            P("lon"),
            P("lon"),
            P("lon"),
        ),
        out_specs=(P("ens", "lon", None), P("lon", None)),
        check_vma=False,
    )
```

```python
import jax
import jax.numpy as jnp
from jax import lax
from jax.experimental import pallas as pl
from jax.experimental.pallas import tpu as pltpu
from jax.sharding import PartitionSpec as P


F32 = jnp.float32
BF16 = jnp.bfloat16
HIGHEST = lax.Precision.HIGHEST
SMEM = pltpu.SMEM
VMEM = pltpu.VMEM

BLOCK = 128
SLOT = 64
NT = (((1,), (1,)), ((), ()))
TN = (((0,), (0,)), ((), ()))


def vmem(*shape_dtype):
    return pl.BlockSpec(memory_space=VMEM)


def smem():
    return pl.BlockSpec(memory_space=SMEM)


def position(pieces_x):
    lon = lax.axis_index("lon")
    return lon % 2, lax.axis_index("ens"), lon // (lax.axis_size("lon") // pieces_x)


def widen(index_ref, pert_ref, eig_ref, wide, lane):
    members, lon_cols, _ = pert_ref.shape
    cut = slice(lane * 128, (lane + 1) * 128)
    for member in range(members):
        wide[lane, member * lon_cols : (member + 1) * lon_cols, :] = pert_ref[member, :, cut].astype(F32)
    for mode in range(index_ref.shape[0]):
        at = (members + mode) * lon_cols
        wide[lane, at : at + lon_cols, :] = eig_ref[index_ref[mode], :, cut].astype(F32)
    return cut


def edge_body(index_ref, pert_ref, eig_ref, mean_ref, edge_ref, wide):
    members, lon_cols, lat = pert_ref.shape
    slot = members + index_ref.shape[0]
    for lane in range(lat // 128):
        cut = widen(index_ref, pert_ref, eig_ref, wide, lane)
        edge_ref[:slot, cut] = wide[lane, pl.ds(0, slot, stride=lon_cols), :].astype(BF16)
    rest = edge_ref.shape[0] - slot
    mean_row = mean_ref[0:1, :].astype(F32)
    edge_ref[slot:, :] = jnp.broadcast_to(mean_row, (rest, lat)).astype(BF16)


def table_body(index_ref, pert_ref, eig_ref, table_ref, wide):
    members, lon_cols, lat = pert_ref.shape
    slot = members + index_ref.shape[0]
    for lane in range(lat // 128):
        cut = widen(index_ref, pert_ref, eig_ref, wide, lane)
        for j in range(lon_cols):
            table_ref[j * slot : (j + 1) * slot, cut] = wide[
                lane, pl.ds(j, slot, stride=lon_cols), :
            ].astype(BF16)


def observe_body(
    sizes, col_ref, row_ref, frac_ref, value_ref, sigma_ref, table_ref, edge_ref, mean_ref,
    keep_ref, send_ref, cells, columns, packed,
):
    members, modes, obs_scale_root, width, pieces_y, pieces_x = sizes
    step = pl.program_id(0)
    steps = pl.num_programs(0)
    lon_cols, lat = mean_ref.shape
    slot = members + modes
    count = members * modes
    mean_at = (lon_cols + 1) * slot

    @pl.when(step == 0)
    def _():
        cells[: lon_cols * slot, :] = table_ref[...]
        cells[lon_cols * slot : mean_at, :] = edge_ref[:slot, :]
        rest = cells.shape[0] - mean_at
        line = lax.broadcasted_iota(jnp.int32, (rest, lat), 0)
        means = jnp.zeros((rest, lat), F32)
        for j in range(lon_cols):
            means = jnp.where(line == j, mean_ref[j : j + 1, :].astype(F32), means)
        means = jnp.where(line == lon_cols, edge_ref[slot : slot + 1, :].astype(F32), means)
        cells[mean_at:, :] = means.astype(BF16)

    at = pl.multiple_of((lax.axis_index("ens") * steps + step) * width, 128)
    col = col_ref[:, pl.ds(at, width)]
    row = row_ref[:, pl.ds(at, width)]
    fraction = frac_ref[:, pl.ds(at, width)]
    observed = value_ref[:, pl.ds(at, width)]
    obs_error = sigma_ref[:, pl.ds(at, width)]
    high = row // 256
    low = row - high * 256
    spread_high = jnp.broadcast_to(high, (16, width))
    spread_low = jnp.broadcast_to(low, (16, width))
    place = lax.broadcasted_iota(jnp.int32, (256, width), 0).astype(F32).astype(BF16)
    one = jnp.ones((256, width), BF16)
    none = jnp.zeros((256, width), BF16)
    chunk = 2
    found = None
    for start in range(0, lat // 256, chunk):
        parts = []
        for part in range(start, start + chunk):
            wanted = jnp.where(spread_high == part, spread_low, -1).astype(F32).astype(BF16)
            parts.append(jnp.where(place == jnp.concatenate([wanted] * 16, axis=0), one, none))
        hot = jnp.concatenate(parts, axis=0)
        piece = jnp.dot(
            cells[:, start * 256 : (start + chunk) * 256], hot, preferred_element_type=F32
        )
        found = piece if found is None else found + piece
    here = found[:slot]
    beyond = found[slot : 2 * slot]
    mean_here = found[mean_at : mean_at + 1]
    mean_next = found[mean_at + 1 : mean_at + 2]
    for j in range(1, lon_cols):
        pick = col == j
        here = jnp.where(pick, found[j * slot : (j + 1) * slot], here)
        beyond = jnp.where(pick, found[(j + 1) * slot : (j + 2) * slot], beyond)
        mean_here = jnp.where(pick, found[mean_at + j : mean_at + j + 1], mean_here)
        mean_next = jnp.where(pick, found[mean_at + j + 1 : mean_at + j + 2], mean_next)
    weight = obs_scale_root / obs_error
    pert_here = here[:members]
    pert_next = beyond[:members]
    mode_here = here[members:] * ((1.0 - fraction) * weight)
    mode_next = beyond[members:] * (fraction * weight)
    normed = (observed - ((1.0 - fraction) * mean_here + fraction * mean_next)) / obs_error
    own = pl.multiple_of(step * width, 128)
    for mode in range(modes):
        block = mode_here[mode : mode + 1] * pert_here + mode_next[mode : mode + 1] * pert_next
        columns[mode * members : (mode + 1) * members, pl.ds(own, width)] = block.astype(BF16)
    normed_high = normed.astype(BF16).astype(F32)
    normed_low = normed - normed_high
    which = lax.broadcasted_iota(jnp.int32, (16, width), 0)
    extra = jnp.where(
        which == 0,
        jnp.broadcast_to(normed_high, (16, width)),
        jnp.where(which == 1, jnp.broadcast_to(normed_low, (16, width)), 0.0),
    )
    columns[count : count + 16, pl.ds(own, width)] = extra.astype(BF16)

    @pl.when(step == steps - 1)
    def _():
        everything = columns[...]
        blocks = count // BLOCK
        tail = lax.dot_general(
            everything[count:], everything, NT, preferred_element_type=F32
        )
        gain = tail[0:1, :count] + tail[1:2, :count]
        own = everything[count:].astype(F32)
        total_normed = own[0:1] + own[1:2]
        square_sum = jnp.sum(total_normed * total_normed)
        row_at = lax.broadcasted_iota(jnp.int32, (BLOCK, BLOCK), 0)
        lane_at = lax.broadcasted_iota(jnp.int32, (BLOCK, BLOCK), 1)
        at_block = 0
        for i in range(blocks):
            strip = lax.dot_general(
                everything[i * BLOCK : (i + 1) * BLOCK],
                everything[: (i + 1) * BLOCK],
                NT,
                preferred_element_type=F32,
            )
            for j in range(i + 1):
                block = strip[:, j * BLOCK : (j + 1) * BLOCK]
                if i == j:
                    part = gain[:, i * BLOCK : (i + 1) * BLOCK]
                    turned = pltpu.roll(jnp.broadcast_to(part, (8, BLOCK)), SLOT, axis=1)
                    upper = lane_at >= SLOT
                    block = jnp.where((row_at == 0) & upper, jnp.broadcast_to(turned[0:1], (BLOCK, BLOCK)), block)
                    block = jnp.where(
                        (row_at == 1) & upper, jnp.broadcast_to(part, (BLOCK, BLOCK)), block
                    )
                    if i == 0:
                        block = jnp.where((row_at == 2) & upper, square_sum, block)
                packed[at_block * BLOCK : (at_block + 1) * BLOCK, :] = block
                at_block += 1
        core, own_y, own_x = position(pieces_x)
        pieces = 2 * pieces_y * pieces_x
        size = packed.shape[0] // pieces
        half = pieces // 2
        for side, out_ref in ((0, keep_ref), (1, send_ref)):
            for slot in range(half):
                y = own_y ^ (slot // pieces_x)
                x = own_x ^ (slot % pieces_x)
                c = core if side == 0 else 1 - core
                piece = (c * pieces_y + y) * pieces_x + x
                out_ref[slot * size : (slot + 1) * size, :] = packed[
                    pl.ds(pl.multiple_of(piece * size, 8), size), :
                ]


def total(terms):
    while len(terms) > 1:
        terms = [terms[i] + terms[i + 1] if i + 1 < len(terms) else terms[i] for i in range(0, len(terms), 2)]
    return terms[0]


def invert_diagonal(work, base):
    tiles = BLOCK // 8
    lane = lax.broadcasted_iota(jnp.int32, (8, BLOCK), 1)
    sub = lax.broadcasted_iota(jnp.int32, (8, BLOCK), 0)
    rows = [work[pl.ds(base + 8 * t, 8), pl.ds(base, BLOCK)] for t in range(tiles)]
    for t in range(tiles):
        at = 8 * t
        mine = rows[t]
        current = [
            [jnp.broadcast_to(mine[i : i + 1, at + j : at + j + 1], (8, BLOCK)) for j in range(i + 1)]
            for i in range(8)
        ]
        outside = {
            s: [jnp.broadcast_to(rows[s][:, at + j : at + j + 1], (8, BLOCK)) for j in range(8)]
            for s in range(t + 1, tiles)
        }
        clear = (lane >= at) & (lane < at + 8)
        base_row = jnp.where(clear, jnp.where(lane - at == sub, 1.0, 0.0), mine)
        done = [jnp.broadcast_to(base_row[k : k + 1, :], (8, BLOCK)) for k in range(8)]
        pivots = []
        roots = []
        inv = [[None] * 8 for _ in range(8)]
        for k in range(0, 8, 2):
            first, cross, second = current[k][k], current[k + 1][k], current[k + 1][k + 1]
            det = first * second - cross * cross
            recip = 1.0 / first
            recip_det = 1.0 / det
            pivots += [recip, first * recip_det]
            roots += [first, det * recip]
            both = recip * recip_det
            turned = {i: first * current[i][k + 1] - cross * current[i][k] for i in range(k + 2, 8)}
            for i in range(k + 2, 8):
                for j in range(k + 2, i + 1):
                    value = current[i][j] - (current[i][k] * current[j][k]) * recip
                    current[i][j] = value - (turned[i] * turned[j]) * both
            for kk in (k, k + 1):
                for i in range(kk + 1, 8):
                    if kk > k:
                        unit = turned[i] * recip_det
                    else:
                        unit = current[i][k] * recip
                    done[i] = done[i] - unit * done[kk]
                    for j in range(kk):
                        inv[i][j] = inv[i][j] - unit * inv[kk][j]
                    inv[i][kk] = -unit
        scaled = [done[i] * pivots[i] for i in range(8)]
        solved = [total([scaled[j]] + [inv[i][j] * scaled[i] for i in range(j + 1, 8)]) for j in range(8)]
        for s in range(t + 1, tiles):
            left = jnp.where(clear, 0.0, rows[s])
            rows[s] = left - total([outside[s][j] * solved[j] for j in range(8)])
        out = done[0] * lax.rsqrt(roots[0])
        for i in range(1, 8):
            out = jnp.where(sub == i, done[i] * lax.rsqrt(roots[i]), out)
        rows[t] = jnp.where(lane < at + 8, out, 0.0)
    return rows


def factor_body(sizes, parts_ref, inverse_ref, scale_ref, packed, corner, full):
    pieces_y, pieces_x, obs_total, members = sizes
    core, own_y, own_x = position(pieces_x)
    pieces = 2 * pieces_y * pieces_x
    size = packed.shape[0] // pieces
    half = pieces // 2
    for side in range(2):
        for slot in range(half):
            y = own_y ^ (slot // pieces_x)
            x = own_x ^ (slot % pieces_x)
            c = core if side == 0 else 1 - core
            piece = (c * pieces_y + y) * pieces_x + x
            packed[pl.ds(pl.multiple_of(piece * size, 8), size), :] = parts_ref[
                (side * half + slot) * size : (side * half + slot + 1) * size, :
            ].astype(F32)
    count = full.shape[0]
    blocks = count // BLOCK
    row_at = lax.broadcasted_iota(jnp.int32, (BLOCK, BLOCK), 0)
    lane_at = lax.broadcasted_iota(jnp.int32, (BLOCK, BLOCK), 1)
    square_sum = packed[2:3, SLOT : SLOT + 1]
    prior_scale = 2.0 / (1.0 + square_sum / obs_total)
    gains = []
    at_block = 0
    for i in range(blocks):
        for j in range(i + 1):
            block = packed[at_block * BLOCK : (at_block + 1) * BLOCK, :]
            at_block += 1
            if i == j:
                first = pltpu.roll(jnp.broadcast_to(block[0:1], (8, BLOCK)), SLOT, axis=1)[0:1]
                gains.append(jnp.where(lane_at[0:1] < SLOT, first, block[1:2]))
                block = jnp.where(row_at >= lane_at, block, block.T)
                block = block * prior_scale + jnp.where(row_at == lane_at, 1.0, 0.0)
                full[i * BLOCK : (i + 1) * BLOCK, j * BLOCK : (j + 1) * BLOCK] = block
            else:
                block = block * prior_scale
                full[j * BLOCK : (j + 1) * BLOCK, i * BLOCK : (i + 1) * BLOCK] = block.T
    def eliminate(b):
        low, high = b * BLOCK, (b + 1) * BLOCK
        diag = corner[...]
        if b > 0:
            left = jnp.dot(diag, full[low:high, :low], precision=HIGHEST, preferred_element_type=F32)
        if high < count:
            right = jnp.dot(diag, full[low:high, high:], precision=HIGHEST, preferred_element_type=F32)
            for i in range(b + 1, blocks):
                ilow, ihigh = i * BLOCK, (i + 1) * BLOCK
                factor = right[:, ilow - high : ihigh - high]
                full[ilow:ihigh, ilow:] = full[ilow:ihigh, ilow:] - lax.dot_general(
                    factor, right[:, ilow - high :], TN, precision=HIGHEST, preferred_element_type=F32
                )
                if b > 0:
                    full[ilow:ihigh, :low] = full[ilow:ihigh, :low] - lax.dot_general(
                        factor, left, TN, precision=HIGHEST, preferred_element_type=F32
                    )
                full[ilow:ihigh, low:high] = -lax.dot_general(
                    factor, diag, TN, precision=HIGHEST, preferred_element_type=F32
                )
            full[low:high, high:] = jnp.zeros((BLOCK, count - high), F32)
        full[low:high, low:high] = diag
        if b > 0:
            full[low:high, :low] = left

    def advance(b, carry):
        rows = invert_diagonal(full, pl.multiple_of(b * BLOCK, BLOCK))
        for t, row in enumerate(rows):
            corner[8 * t : 8 * t + 8, :] = row
        for k in range(blocks):
            pl.when(b == k)(lambda k=k: eliminate(k))
        return carry

    lax.fori_loop(0, blocks, advance, 0)
    inverse = full[...]
    gain = jnp.broadcast_to(jnp.concatenate(gains, axis=1), (8, count))
    inner = lax.dot_general(gain, inverse, NT, precision=HIGHEST, preferred_element_type=F32)
    weights = jnp.dot(inner, inverse, precision=HIGHEST, preferred_element_type=F32)
    weights = weights * jnp.sqrt(prior_scale)
    own_rows = inverse_ref.shape[0] - 16
    inverse_ref[:own_rows, :] = full[pl.ds(pl.multiple_of(own_y * own_rows, 8), own_rows), :].astype(BF16)
    inverse_ref[own_rows:, :] = jnp.broadcast_to(weights[0:1], (16, count)).astype(BF16)
    scale_ref[...] = jnp.broadcast_to(prior_scale, scale_ref.shape)


def apply_body(sizes, scale_ref, inverse_ref, table_ref, analysis_ref, increment_ref, columns, wide):
    members, modes, lon_cols, inv_root = sizes
    own_rows = analysis_ref.shape[0]
    prior_scale = scale_ref[0:1, 0:1]
    analysis_scale = jnp.sqrt(prior_scale * (members - 1)) * inv_root
    increment_scale = jnp.sqrt(prior_scale) * inv_root
    for j in range(lon_cols):
        base = j * (members + modes)
        own = table_ref[base : base + members, :]
        picked = table_ref[base + members : base + members + modes, :]
        for mode in range(modes):
            columns[mode * members : (mode + 1) * members, :] = picked[mode : mode + 1] * own
        product = jnp.dot(inverse_ref[...], columns[...], preferred_element_type=F32)
        for lane in range(wide.shape[0]):
            cut = slice(lane * 128, (lane + 1) * 128)
            wide[lane, pl.ds(j, own_rows, stride=lon_cols), :] = product[:own_rows, cut] * analysis_scale
        increment_ref[j : j + 1, :] = product[own_rows : own_rows + 1] * increment_scale
    for lane in range(wide.shape[0]):
        cut = slice(lane * 128, (lane + 1) * 128)
        analysis_ref[:, :, cut] = wide[lane].astype(BF16).reshape(own_rows, lon_cols, 128)


def local(perturb, eig_table, mode_index, mean_state, obs_col, obs_row, obs_frac, obs_value, obs_sigma):
    members, lon_cols, lat = perturb.shape
    table_rows = eig_table.shape[0]
    modes = mode_index.shape[0]
    obs_local = obs_col.shape[0]
    lon_devices = lax.axis_size("lon")
    ens_devices = lax.axis_size("ens")
    obs_total = obs_local * lon_devices
    count = modes * members
    obs_own = obs_local // ens_devices
    xs = 4
    zs = lon_devices // (2 * xs)
    inv_root = 1.0 / float(members - 1) ** 0.5
    obs_scale = (4.0 * members / obs_total) ** 0.5

    slot = members + modes
    cells = 2048
    edge_rows = slot + 8
    edge = pl.pallas_call(
        edge_body,
        grid=(lat // cells,),
        out_shape=jax.ShapeDtypeStruct((edge_rows, lat), BF16),
        in_specs=[
            smem(),
            pl.BlockSpec((members, lon_cols, cells), lambda g: (0, 0, g)),
            pl.BlockSpec((table_rows, lon_cols, cells), lambda g: (0, 0, g)),
            pl.BlockSpec((lon_cols, cells), lambda g: (0, g)),
        ],
        out_specs=pl.BlockSpec((edge_rows, cells), lambda g: (0, g)),
        scratch_shapes=[VMEM((cells // 128, slot * lon_cols, 128), F32)],
        name="edge",
    )(mode_index, perturb, eig_table, mean_state)
    back = [(source, (source - 1) % lon_devices) for source in range(lon_devices)]
    edge = lax.ppermute(edge, "lon", back)
    table = pl.pallas_call(
        table_body,
        grid=(lat // cells,),
        out_shape=jax.ShapeDtypeStruct((lon_cols * slot, lat), BF16),
        in_specs=[
            smem(),
            pl.BlockSpec((members, lon_cols, cells), lambda g: (0, 0, g)),
            pl.BlockSpec((table_rows, lon_cols, cells), lambda g: (0, 0, g)),
        ],
        out_specs=pl.BlockSpec((lon_cols * slot, cells), lambda g: (0, g)),
        scratch_shapes=[VMEM((cells // 128, slot * lon_cols, 128), F32)],
        name="table",
    )(mode_index, perturb, eig_table)
    width = 1024
    steps = obs_own // width
    blocks = count // BLOCK
    packed_rows = blocks * (blocks + 1) // 2 * BLOCK
    half = packed_rows // 2
    ys = ens_devices
    keep, send = pl.pallas_call(
        lambda *refs: observe_body((members, modes, obs_scale * inv_root, width, ys, xs), *refs),
        grid=(steps,),
        out_shape=[jax.ShapeDtypeStruct((half, BLOCK), F32)] * 2,
        in_specs=[vmem()] * 8,
        out_specs=[vmem(), vmem()],
        scratch_shapes=[
            VMEM(((lon_cols + 1) * slot + 16, lat), BF16),
            VMEM((count + 16, obs_own), BF16),
            VMEM((packed_rows, BLOCK), F32),
        ],
        name="observe",
    )(
        *[v.reshape(1, obs_local) for v in (obs_col, obs_row, obs_frac, obs_value, obs_sigma)],
        table,
        edge,
        mean_state,
    )

    def at(x, z, c):
        return ((x % xs) * zs + z % zs) * 2 + c

    spots = [(x, z, c) for x in range(xs) for z in range(zs) for c in range(2)]
    over_core = [(at(x, z, c), at(x, z, 1 - c)) for x, z, c in spots]

    def over_x(d):
        return [(at(x, z, c), at(x ^ d, z, c)) for x, z, c in spots]

    def over_z(d):
        return [(at(x, z, c), at(x, z ^ d, c)) for x, z, c in spots]

    def over_y(d):
        return [(y, y ^ d) for y in range(ys)]

    quarter = half // ys
    piece = quarter // xs
    got = lax.ppermute(send, "lon", over_core)
    mine = keep + got
    got = [lax.ppermute(mine[d * quarter : (d + 1) * quarter], "ens", over_y(d)) for d in range(1, ys)]
    mine = mine[:quarter] + sum(got)
    got = [lax.ppermute(mine[d * piece : (d + 1) * piece], "lon", over_x(d)) for d in range(1, xs)]
    mine = mine[:piece] + sum(got)
    for d in (1, 2, 6):
        mine = mine + lax.ppermute(mine, "lon", over_z(d))
    got = [lax.ppermute(mine, "lon", over_x(d)) for d in range(1, xs)]
    mine = jnp.concatenate([mine] + got)
    got = [lax.ppermute(mine, "ens", over_y(d)) for d in range(1, ys)]
    mine = jnp.concatenate([mine] + got)
    got = lax.ppermute(mine, "lon", over_core)
    parts = jnp.concatenate([mine, got])

    own_columns = count // ens_devices
    inverse, scale = pl.pallas_call(
        lambda *refs: factor_body((ys, xs, float(obs_total), members), *refs),
        out_shape=[
            jax.ShapeDtypeStruct((own_columns + 16, count), BF16),
            jax.ShapeDtypeStruct((8, 128), F32),
        ],
        in_specs=[vmem()],
        out_specs=[vmem(), vmem()],
        scratch_shapes=[VMEM((packed_rows, BLOCK), F32), VMEM((BLOCK, BLOCK), F32), VMEM((count, count), F32)],
        name="factor",
    )(parts)
    cells = 1024
    analysis, increment = pl.pallas_call(
        lambda *refs: apply_body((members, modes, lon_cols, inv_root), *refs),
        grid=(lat // cells,),
        out_shape=[
            jax.ShapeDtypeStruct((own_columns, lon_cols, lat), BF16),
            jax.ShapeDtypeStruct((lon_cols, lat), F32),
        ],
        in_specs=[
            vmem(),
            vmem(),
            pl.BlockSpec((lon_cols * slot, cells), lambda g: (0, g)),
        ],
        out_specs=[
            pl.BlockSpec((own_columns, lon_cols, cells), lambda g: (0, 0, g)),
            pl.BlockSpec((lon_cols, cells), lambda g: (0, g)),
        ],
        scratch_shapes=[VMEM((count, cells), BF16), VMEM((cells // 128, own_columns * lon_cols, 128), F32)],
        name="apply",
    )(scale, inverse, table)
    return (analysis, increment)


def solution(mesh):
    return jax.shard_map(
        local,
        mesh=mesh,
        in_specs=(
            P(None, "lon", None),
            P(None, "lon", None),
            P(),
            P("lon", None),
            P("lon"),
            P("lon"),
            P("lon"),
            P("lon"),
            P("lon"),
        ),
        out_specs=(P("ens", "lon", None), P("lon", None)),
        check_vma=False,
    )
```
